128 devices in a mesh: section: 2 (over x_hi), expert: 16 (over z, y), tensor: 4 (over x_lo, core).
Axes of the slice: x: 4 (x_hi: 2, x_lo: 2; x = x_hi * 2 + x_lo), y: 4, z: 4, core: 2. Of those that a mesh axis runs over, the one named last changes fastest.
Arguments:
- layer_inputs: bfloat16 [2, 2, 1280, 3072], P('section', None, 'expert', 'tensor'), may hold values from -6 to 6
- grad_out: bfloat16 [2, 1280, 3072], P(None, 'expert', 'tensor'), may hold values from -6 to 6
- norm_gain: bfloat16 [2, 3072], P('section', 'tensor'), may hold values from 0.25 to 1.75
- router_w: bfloat16 [2, 3072, 4], P('section', 'tensor'), may hold values from -0.21875 to 0.21875
- w_gate: bfloat16 [2, 3072, 32768], P('section', None, ('expert', 'tensor')), may hold values from -0.109375 to 0.109375
- w_up: bfloat16 [2, 3072, 32768], P('section', None, ('expert', 'tensor')), may hold values from -0.109375 to 0.109375
- w_down: bfloat16 [2, 32768, 3072], P('section', ('expert', 'tensor')), may hold values from -0.0625 to 0.0625
- saved_gate: bfloat16 [2, 2, 16, 64, 32768], P('section', None, None, None, ('expert', 'tensor')), may hold values from -6 to 6
- saved_up: bfloat16 [2, 2, 16, 64, 32768], P('section', None, None, None, ('expert', 'tensor')), may hold values from -6 to 6
- routes: int32 [2, 2, 1280, 2], P('section', None, 'expert'), may hold values from 0 to 3, all different within a row; in each aligned block of 80 rows (0 to 79, 80 to 159, ..., all dimensions but the last counted through in order) at most 64 rows name the same one
Outputs:
- layer_grads: bfloat16 [2, 2, 1280, 3072], P('section', None, 'expert', 'tensor')
The draws below stay inside these ranges and needn't reach their ends.
Inputs may be any that keep to these rules, and one draw needn't show every extreme that they name: `routes`: each token names two different experts; within the 80 tokens of one device's aligned block of a layer and micro-batch, no expert is named by more than 64 tokens, and in some blocks one expert is named by exactly 64.
All inputs are finite; a program needn't handle non-finite values.
Results may differ from the reference program's by a relative error of at most 0.011.
Values may be sent and summed in bfloat16 or wider, within the bound.
A program may use at most 128 MiB of HBM per device.

```python
import math
import jax
import jax.numpy as jnp
import numpy as np
from jax import lax

D = 3072
FF = 8192
EXPERTS = 4
TOP = 2
MICRO = 2
TOK_DEV = 80
CAP = 64
LAYERS = 2
TOKENS = 1280
N_EXPERT = 16


def levels(own_key, dims, cuts, low, largest):
    def one(dim, parts):
        steps = jax.random.uniform(jax.random.fold_in(jax.random.fold_in(own_key, 6), dim), (parts,), jnp.float32, low / len(cuts), largest / len(cuts))
        return jnp.repeat(jnp.exp(steps), dims[dim] // parts).reshape((-1,) + (1,) * (len(dims) - dim - 1))

    loudness = one(*cuts[0])
    for cut in cuts[1:]:
        loudness = loudness * one(*cut)
    return loudness


def deal_out(own_key, own, number, rows, count, top, most, lean):
    ranking = jax.random.permutation(own_key, count)
    crowded, common = portions_of(count, rows * top, most, lean, True), portions_of(count, rows * top, most, lean, False)
    places = jnp.arange(count)

    def named(sizes, turn):
        used = int((sizes > 0).sum())
        fixed = max(1, used // 4)
        shifted = fixed + (places - fixed + turn * (used - fixed)) % max(1, count - fixed)
        return jnp.zeros((count,), jnp.int32).at[ranking[jnp.where(places < fixed, places, shifted)]].set(jnp.asarray(sizes, jnp.int32))

    sizes = jnp.where(number % 4 == 0, named(crowded, number // 4), named(common, number - number // 4 - 1))
    mixed = jax.random.permutation(jax.random.fold_in(own, 3), count)
    source_of, receiver = mixed[0:count // 2 * 2:2], mixed[1:count // 2 * 2:2]
    slack = jnp.minimum(sizes[source_of] - 1, most - sizes[receiver]) // 2
    slack = jnp.where((source_of == ranking[0]) | (receiver == ranking[0]) | (sizes[receiver] == 0), 0, jnp.maximum(slack, 0))
    shifted = jax.random.randint(jax.random.fold_in(own, 4), (count // 2,), 0, 1 << 20) % (slack + 1)
    sizes = sizes.at[source_of].add(-shifted).at[receiver].add(shifted)
    labels = jnp.searchsorted(jnp.cumsum(sizes), jnp.arange(rows * top), side="right").astype(jnp.int32)
    grid = labels.reshape(top, rows).T
    grid = grid[jax.random.permutation(jax.random.fold_in(own, 1), rows)]
    turn = jax.random.randint(jax.random.fold_in(own, 2), (rows, 1), 0, top)
    return jnp.take_along_axis(grid, (jnp.arange(top)[None, :] + turn) % top, axis=1)


def portions_of(number_of, total, limit, skew, full):
    loads = [(1 << 20) // math.isqrt(rank ** skew) + 1 for rank in range(1, number_of + 1)]
    largest = limit if full else min(limit, max(-(-total // number_of), total * loads[0] // sum(loads)))
    least = 1 if total - largest >= number_of - 1 else 0
    given, surplus = [largest] + [least] * (number_of - 1), total - largest - least * (number_of - 1)
    while surplus > 0:
        free = [i for i in range(1, number_of) if given[i] < largest] or [i for i in range(1, number_of) if given[i] < limit]
        whole, left = sum([loads[i] for i in free]), surplus
        for i in free:
            addition = min(limit - given[i], max(1, left * loads[i] // whole), surplus)
            given[i] = given[i] + addition
            surplus = surplus - addition
    return np.array(given)


def scatter_about(rng, dims, spread, bound, split=(), kind=jnp.bfloat16):
    array = spread * jax.random.normal(rng, dims, jnp.float32)
    if split:
        array = array * levels(rng, dims, split, -0.22, 0.18)
    return jnp.clip(array, -bound, bound).astype(kind)


def setup_inputs(seed: int = 0) -> dict:
    key_list = jax.random.split(jax.random.key(seed), 11)
    layer_inputs = scatter_about(key_list[0], (LAYERS, MICRO, TOKENS, D), 1.0, 6.0, ((0, 2), (2, 16), (3, 4)))
    grad_out = scatter_about(key_list[1], (MICRO, TOKENS, D), 1.0, 6.0, ((1, 16), (2, 4)))
    norm_gain = jnp.clip(1.0 + 0.15 * jax.random.normal(key_list[2], (LAYERS, D), jnp.float32), 0.25, 1.75).astype(jnp.bfloat16)
    router_w = scatter_about(key_list[3], (LAYERS, D, EXPERTS), (D // 4) ** -0.5, 0.21875, ((0, 2), (1, 4)))
    w_gate = scatter_about(key_list[4], (LAYERS, D, EXPERTS * FF), D ** -0.5, 0.109375, ((0, 2), (2, 64)))
    w_up = scatter_about(key_list[5], (LAYERS, D, EXPERTS * FF), D ** -0.5, 0.109375, ((0, 2), (2, 64)))
    w_down = scatter_about(key_list[6], (LAYERS, EXPERTS * FF, D), FF ** -0.5, 0.0625, ((0, 2), (1, 64)))
    saved_gate = scatter_about(key_list[7], (LAYERS, MICRO, N_EXPERT, CAP, EXPERTS * FF), 1.0, 6.0, ((0, 2), (4, 64)))
    saved_up = scatter_about(key_list[8], (LAYERS, MICRO, N_EXPERT, CAP, EXPERTS * FF), 1.0, 6.0, ((0, 2), (4, 64)))
    routes_keys = jax.random.split(jax.random.fold_in(key_list[9], 1), LAYERS * MICRO * TOKENS // TOK_DEV)
    routes_turns = jax.random.permutation(jax.random.fold_in(key_list[9], 3), LAYERS * MICRO * TOKENS // TOK_DEV)
    routes = jax.vmap(lambda own, number: deal_out(jax.random.fold_in(key_list[9], 2), own, number, TOK_DEV, EXPERTS, TOP, CAP, 2))(routes_keys, routes_turns).reshape((LAYERS, MICRO, TOKENS, TOP))
    return {"layer_inputs": layer_inputs, "grad_out": grad_out, "norm_gain": norm_gain, "router_w": router_w, "w_gate": w_gate, "w_up": w_up, "w_down": w_down, "saved_gate": saved_gate, "saved_up": saved_up, "routes": routes}


norm_eps = 1e-05
highest = lax.Precision.HIGHEST

def layer_back(inputs, upstream, gain, router, gate_mats, up_mats, down_mats, gate_saved, up_saved, chosen):
    values = inputs.astype(jnp.float32)
    gain_full = gain.astype(jnp.float32)
    scale = lax.rsqrt(lax.optimization_barrier(jnp.mean(values * values, axis=-1, keepdims=True)) + norm_eps)
    normed = (values * scale * gain_full).astype(jnp.bfloat16)
    logits = jnp.dot(normed, router, preferred_element_type=jnp.float32)
    experts = router.shape[1]
    tokens = values.shape[0]
    senders = tokens // TOK_DEV
    onehot = (chosen[:, :, None] == jnp.arange(experts, dtype=jnp.int32)[None, None, :]).astype(jnp.float32)
    picked = lax.optimization_barrier(jnp.sum(onehot * logits[:, None, :], axis=-1))
    first = jax.nn.sigmoid(picked[:, 0] - picked[:, 1])
    second = jax.nn.sigmoid(picked[:, 1] - picked[:, 0])
    blocks = onehot.reshape(senders, TOK_DEV * 2, experts)
    earlier = jnp.cumsum(blocks, axis=1) - blocks
    within = lax.optimization_barrier(jnp.sum(earlier * blocks, axis=-1)).astype(jnp.int32).reshape(tokens, 2)
    sender = jnp.arange(tokens, dtype=jnp.int32) // TOK_DEV
    token_ids = jnp.arange(tokens, dtype=jnp.int32)
    slot_total = senders * CAP
    hidden_grad = jnp.zeros(values.shape, jnp.float32)
    prob_grad = jnp.zeros(picked.shape, jnp.float32)
    for expert in range(experts):
        mine = chosen == expert
        used = jnp.any(mine, axis=1)
        place_at = lax.optimization_barrier(jnp.sum(jnp.where(mine, within, 0), axis=1)).astype(jnp.int32)
        slot = jnp.where(used, sender * CAP + place_at, slot_total).astype(jnp.int32)
        table = jnp.zeros((slot_total + 1,), jnp.int32).at[slot].set(token_ids)[:-1]
        filled = jnp.zeros((slot_total + 1,), jnp.int32).at[slot].set(1)[:-1]
        rows = jnp.where(filled[:, None] > 0, upstream[table], jnp.zeros((), jnp.bfloat16))
        low = expert * FF
        gate_act = gate_saved[:, :, low:low + FF].reshape(slot_total, FF).astype(jnp.float32)
        up_act = up_saved[:, :, low:low + FF].reshape(slot_total, FF).astype(jnp.float32)
        back_act = jnp.dot(rows, down_mats[low:low + FF].T, preferred_element_type=jnp.float32)
        sigma = jax.nn.sigmoid(gate_act)
        swish = gate_act * sigma
        weight_grad = lax.optimization_barrier(jnp.sum(swish * up_act * back_act, axis=-1))
        slope = sigma * (1.0 + gate_act * (1.0 - sigma))
        gate_grad = (back_act * up_act * slope).astype(jnp.bfloat16)
        up_grad = (back_act * swish).astype(jnp.bfloat16)
        unit = jnp.dot(gate_grad, gate_mats[:, low:low + FF].T, preferred_element_type=jnp.float32)
        unit = unit + jnp.dot(up_grad, up_mats[:, low:low + FF].T, preferred_element_type=jnp.float32)
        reach = jnp.minimum(slot, slot_total - 1).astype(jnp.int32)
        share = first * onehot[:, 0, expert] + second * onehot[:, 1, expert]
        hidden_grad = hidden_grad + share[:, None] * unit[reach]
        prob_grad = prob_grad + onehot[:, :, expert] * weight_grad[reach][:, None]
    logit_step = first * second * (prob_grad[:, 0] - prob_grad[:, 1])
    logit_grad = (onehot[:, 0, :] - onehot[:, 1, :]) * logit_step[:, None]
    hidden_grad = hidden_grad + jnp.dot(logit_grad, router.astype(jnp.float32).T, precision=highest)
    gained = hidden_grad * gain_full
    moment = lax.optimization_barrier(jnp.mean(values * gained, axis=-1, keepdims=True))
    result = upstream.astype(jnp.float32) + scale * gained - values * scale * scale * scale * moment
    return result.astype(jnp.bfloat16)

def reference(layer_inputs, grad_out, norm_gain, router_w, w_gate, w_up, w_down, saved_gate, saved_up, routes):
    stacked = []
    for micro in range(MICRO):

        def one_layer(upstream, pieces):
            inputs, gain, router, gate_mats, up_mats, down_mats, gate_saved, up_saved, chosen = pieces
            result = layer_back(inputs, upstream, gain, router, gate_mats, up_mats, down_mats, gate_saved, up_saved, chosen)
            return (result, result)
        pieces = (layer_inputs[:, micro], norm_gain, router_w, w_gate, w_up, w_down, saved_gate[:, micro], saved_up[:, micro], routes[:, micro])
        final, series = lax.scan(one_layer, grad_out[micro], pieces, reverse=True)
        stacked.append(series)
    return jnp.stack(stacked, axis=1)
```

```python
import functools
import jax
import jax.numpy as jnp
from jax import lax
from jax.experimental import pallas as pl
from jax.experimental.pallas import tpu as pltpu
from jax.sharding import PartitionSpec as P

norm_eps = 1e-05
OFF = (0, -1, 1, 2)
MESH = pl.DeviceIdType.MESH
NT = (((1,), (1,)), ((), ()))


def kernel(
    sections, n, sizes,
    gout, xin, scale, gain, info_h, sg_h, su_h, wd_h, wg_h, wu_h, rp_h,
    out,
    G, U, D, RH, RF, RHF, RFF, RX, hop, mrecv, msend,
    V, A, B, bt, DC, wd, wc, info, sg, su,
    ld, x_s, x_r, fo_s, fo_r, ff_s, ff_r, so_s, so_r, sf_s, sf_r, dd_s, dd_r,
    e_s, e_r, rh_s, rh_r, rf_s, rf_r, hf_s, hf_r, ff2_s, ff2_r, rx_s, rx_r,
    m_s, m_r, hop_s, hop_r, gate,
):
    micros, T, Q, F, cap, lanes = sizes
    width = 4 * Q
    K = 2 * F + lanes
    sec = lax.axis_index("section")
    ex = lax.axis_index("expert")
    te = lax.axis_index("tensor")
    z, y = ex // n, ex % n
    xl, c = te // 2, te % 2
    fp = y * (1 - c) + z * c
    sp = z * (1 - c) + y * c

    def at(v, o):
        return lax.rem(v + o + n, n)

    def exid(f, s):
        return (1 - c) * (s * n + f) + c * (f * n + s)

    partner = {"tensor": xl * 2 + 1 - c}
    xnbr = {"tensor": (1 - xl) * 2 + c}
    xdiag = {"tensor": (1 - xl) * 2 + 1 - c}
    fdir = ({"expert": exid(at(fp, 1), sp)}, {"expert": exid(at(fp, -1), sp)})
    sdir = ({"expert": exid(fp, at(sp, 1))}, {"expert": exid(fp, at(sp, -1))})
    hoppeer = {"section": 1 - sec, "tensor": (1 - xl) * 2 + c}
    near = (partner, xnbr, xdiag) + fdir + sdir

    def load(k, src, dst):
        return pltpu.make_async_copy(src, dst, ld.at[k])

    def weight_loads():
        return (
            load(0, wd_h, wd),
            load(1, wg_h, wc.at[:, pl.ds(0, F)]),
            load(2, wu_h, wc.at[:, pl.ds(F, F)]),
            load(3, rp_h, wc.at[:, pl.ds(2 * F, lanes)]),
        )

    for cp in weight_loads():
        cp.start()

    barrier = pltpu.get_barrier_semaphore()
    greeted = near + ((hoppeer,) if sections == 2 else ())
    for peer in greeted:
        pl.semaphore_signal(barrier, inc=1, device_id=peer, device_id_type=MESH)
    pl.semaphore_wait(barrier, len(greeted))

    def rc(src, dst, ss, rs, peer):
        return pltpu.make_async_remote_copy(
            src_ref=src, dst_ref=dst, send_sem=ss, recv_sem=rs, device_id=peer, device_id_type=MESH
        )

    def one_micro(m, carry):
        @pl.when(m > 0)
        def _():
            for peer in near:
                pl.semaphore_signal(gate, inc=1, device_id=peer, device_id_type=MESH)
            pl.semaphore_wait(gate, len(near))

        small = (
            load(4, info_h.at[m], info),
            load(5, sg_h.at[m], sg),
            load(6, su_h.at[m], su),
        )
        for cp in small:
            cp.start()
        sent = []

        def go(*a):
            cp = rc(*a)
            cp.start()
            sent.append(cp)

        def got(ref, ss, rs, peer):
            rc(ref, ref, ss, rs, peer).wait_recv()

        top = sec == sections - 1
        qh = jnp.where(top, xl, 1 - xl)
        qo = 1 - qh
        mine = G.at[c, sp, fp]

        @pl.when(top)
        def _():
            G[c, sp, fp, qh] = gout[m]

        if sections == 2:

            @pl.when(jnp.logical_not(top))
            def _():
                got(hop.at[m], hop_s.at[m], hop_r.at[m], hoppeer)
                G[c, sp, fp, qh] = hop[m]

        go(mine.at[qh], mine.at[qh], x_s, x_r, xnbr)
        for d in range(2):
            go(mine.at[qh], mine.at[qh], fo_s.at[0, d], fo_r.at[0, d], fdir[d])
        V[...] = jnp.zeros_like(V)
        got(mine.at[qo], x_s, x_r, xnbr)
        for d in range(2):
            go(mine.at[qo], mine.at[qo], fo_s.at[1, d], fo_r.at[1, d], fdir[d])

        def spread(k, slot):
            for d in range(2):
                go(slot, slot, so_s.at[k, d], so_r.at[k, d], sdir[d])

        def share(kk, k, slot):
            go(slot, slot, dd_s.at[kk, k], dd_r.at[kk, k], partner)

        spread(0, mine)
        share(0, 0, mine)
        for cp in small:
            cp.wait()

        @pl.when(m == 0)
        def _():
            for cp in weight_loads():
                cp.wait()

        def prepare(j, carry):
            i0, i1 = j // n, j % n
            pos = info[i0, i1, :, 0:1]
            slots = lax.broadcasted_iota(jnp.int32, (T, cap), 1).astype(jnp.float32)
            place = jnp.where(slots == pos, 1.0, 0.0).astype(jnp.bfloat16)
            a = jnp.dot(place, sg[j], preferred_element_type=jnp.float32)
            b = jnp.dot(place, su[j], preferred_element_type=jnp.float32)
            sig = jax.nn.sigmoid(a)
            A[i0, i1] = b * sig * (1.0 + a * (1.0 - sig))
            B[i0, i1] = a * sig
            bt[i0, i1] = b.astype(jnp.bfloat16)
            return carry

        def prepare_rows(i):
            lax.fori_loop(i * n, (i + 1) * n, prepare, 0)

        def into_v(kk):
            for k in range(n):
                ref = G.at[1 - c, at(fp, OFF[kk]), at(sp, OFF[k])]
                got(ref, dd_s.at[kk, k], dd_r.at[kk, k], partner)
            zi, yi = at(z, OFF[kk]), at(y, OFF[kk])
            for h in range(2):
                part = jnp.zeros((n * T, F), jnp.float32)
                for q in range(2):
                    g = (G[0, zi, :, q] if h == 0 else G[1, yi, :, q]).reshape(n * T, Q)
                    w = wd[:, (2 * q + h) * Q : (2 * q + h + 1) * Q]
                    part = part + lax.dot_general(g, w, NT, preferred_element_type=jnp.float32)
                part = part.reshape(n, T, F)
                if h == 0:
                    V[zi] += part
                else:
                    V[:, yi] += part

        prepare_rows(0)
        for d in range(2):
            f = at(fp, -1 if d == 0 else 1)
            slot = G.at[c, sp, f]
            for i, q in enumerate((qh, qo)):
                got(slot.at[q], fo_s.at[i, d], fo_r.at[i, d], fdir[d])
            go(slot.at[d], slot.at[d], ff_s.at[d], ff_r.at[d], fdir[d])
            spread(1 + d, slot)
            share(0, 1 + d, slot)
        far = G.at[c, sp, at(fp, 2)]
        for d in range(2):
            got(far.at[d], ff_s.at[d], ff_r.at[d], fdir[d])
        spread(3, far)
        share(0, 3, far)

        def pass_on(k):
            f = at(fp, OFF[k])
            for d in range(2):
                slot = G.at[c, at(sp, -1 if d == 0 else 1), f]
                got(slot, so_s.at[k, d], so_r.at[k, d], sdir[d])
                go(slot.at[d], slot.at[d], sf_s.at[k, d], sf_r.at[k, d], sdir[d])
                share(1 + d, k, slot)

        pass_on(0)
        prepare_rows(1)
        pass_on(1)
        into_v(0)
        pass_on(2)
        prepare_rows(2)
        pass_on(3)
        prepare_rows(3)
        for k in range(n):
            slot = G.at[c, at(sp, 2), at(fp, OFF[k])]
            for d in range(2):
                got(slot.at[d], sf_s.at[k, d], sf_r.at[k, d], sdir[d])
            share(3, k, slot)
            if k == 1:
                into_v(1)
            if k == 2:
                into_v(2)
        into_v(3)

        def finish(j, carry):
            i0, i1 = j // n, j % n
            v = V[i0, i1]
            db = v * B[i0, i1]
            w = jnp.sum(db * bt[i0, i1].astype(jnp.float32), axis=-1, keepdims=True)
            row = info[i0, i1]
            DC[i0, i1, :, 0:F] = (v * A[i0, i1]).astype(jnp.bfloat16)
            DC[i0, i1, :, F : 2 * F] = db.astype(jnp.bfloat16)
            DC[i0, i1, :, 2 * F :] = (w * row[:, 2:3] * row).astype(jnp.bfloat16)
            return carry

        lax.fori_loop(0, n * n, finish, 0)

        def into_u(kk):
            zi, yi = at(z, OFF[kk]), at(y, OFF[kk])
            for h in range(2):
                da = (DC[zi] if h == 0 else DC[:, yi]).reshape(n * T, K)
                q_own = (info[zi, :, :, 1:2] if h == 0 else info[:, yi, :, 1:2]).reshape(n * T, 1)

                def half(q, carry):
                    low = pl.multiple_of((2 * q + h) * Q, Q)
                    u = lax.dot_general(
                        da, wc[pl.ds(low, Q), :], NT, preferred_element_type=jnp.float32
                    )
                    u = (u * q_own).astype(jnp.bfloat16).reshape(n, T, Q)
                    U[h, zi if h == 0 else yi, :, q] = u
                    return carry

                lax.fori_loop(0, 2, half, 0)
            go(U.at[1 - c, at(fp, OFF[kk])], D.at[kk], e_s.at[kk], e_r.at[kk], partner)

        def add_partner(kk):
            got(D.at[kk], e_s.at[kk], e_r.at[kk], partner)
            i = at(sp, OFF[kk])
            U[c, i] = U[c, i] + D[kk]

        into_u(3)
        add_partner(3)
        s2 = at(sp, 2)
        for d in range(2):
            go(U.at[c, s2, :, d], RH.at[d], rh_s.at[d], rh_r.at[d], sdir[d])
        into_u(2)
        add_partner(2)
        into_u(1)
        add_partner(1)
        for d in range(2):
            i = at(sp, 1 if d == 0 else -1)
            got(RH.at[d], rh_s.at[d], rh_r.at[d], sdir[d])
            U[c, i, :, d] = U[c, i, :, d] + RH[d]
            for k in (3, 2, 1, 0):
                f = at(fp, OFF[k])
                go(U.at[c, i, f], RF.at[d, k], rf_s.at[d, k], rf_r.at[d, k], sdir[d])
        into_u(0)
        add_partner(0)

        def own_sum(k):
            for d in range(2):
                got(RF.at[d, k], rf_s.at[d, k], rf_r.at[d, k], sdir[d])
            f = at(fp, OFF[k])
            total = U[c, sp, f].astype(jnp.float32) + RF[0, k].astype(jnp.float32)
            U[c, sp, f] = (total + RF[1, k].astype(jnp.float32)).astype(jnp.bfloat16)

        own_sum(3)
        f2 = at(fp, 2)
        for d in range(2):
            go(U.at[c, sp, f2, d], RHF.at[d], hf_s.at[d], hf_r.at[d], fdir[d])
        for d, k in ((0, 2), (1, 1)):
            own_sum(k)
            f = at(fp, OFF[k])
            got(RHF.at[d], hf_s.at[d], hf_r.at[d], fdir[d])
            U[c, sp, f, d] = U[c, sp, f, d] + RHF[d]
            go(U.at[c, sp, f], RFF.at[d], ff2_s.at[d], ff2_r.at[d], fdir[d])
        own_sum(0)
        for d in range(2):
            got(RFF.at[d], ff2_s.at[d], ff2_r.at[d], fdir[d])

        def three(q):
            total = U[c, sp, fp, q].astype(jnp.float32) + RFF[0, q].astype(jnp.float32)
            return total + RFF[1, q].astype(jnp.float32)

        U[c, sp, fp, 1 - xl] = three(1 - xl).astype(jnp.bfloat16)
        go(U.at[c, sp, fp, 1 - xl], RX, rx_s, rx_r, xnbr)
        dn = three(xl)
        got(RX, rx_s, rx_r, xnbr)
        dn = dn + RX[...].astype(jnp.float32)

        gained = dn * gain[...]
        values = xin[m].astype(jnp.float32)
        part = jnp.sum(values * gained, axis=-1, keepdims=True)
        msend[...] = jnp.broadcast_to(part, msend.shape)
        for i, peer in enumerate((partner, xnbr, xdiag)):
            go(msend, mrecv.at[i], m_s.at[i], m_r.at[i], peer)
        for i, peer in enumerate((partner, xnbr, xdiag)):
            got(mrecv.at[i], m_s.at[i], m_r.at[i], peer)
        moment = (msend[...] + mrecv[0] + mrecv[1] + mrecv[2])[:, 0:1] / width
        sc = scale[m][:, 0:1]
        result = G[c, sp, fp, xl].astype(jnp.float32) + sc * gained - values * (sc * sc * sc * moment)
        out[m] = result.astype(jnp.bfloat16)
        if sections == 2:

            @pl.when(top)
            def _():
                rc(out.at[m], hop.at[m], hop_s.at[m], hop_r.at[m], hoppeer).start()

        for cp in sent:
            cp.wait_send()
        if sections == 2:

            @pl.when(top)
            def _():
                rc(out.at[m], hop.at[m], hop_s.at[m], hop_r.at[m], hoppeer).wait_send()

        return carry

    lax.fori_loop(0, micros, one_micro, 0)


def on_device(
    layer_inputs, grad_out, norm_gain, router_w, w_gate, w_up, w_down, saved_gate, saved_up, routes
):
    sections = lax.axis_size("section")
    holders = lax.axis_size("expert")
    n = 4
    micros, T, Q = grad_out.shape
    F = w_gate.shape[2]
    cap = saved_gate.shape[3]
    lanes = 128
    router = router_w[0]
    experts = router.shape[1]
    width = w_gate.shape[1]
    own = lax.axis_index("expert") // (holders // experts)
    gain_full = norm_gain.astype(jnp.float32)
    expert_ids = jnp.arange(experts, dtype=jnp.int32)

    values = layer_inputs[0].astype(jnp.float32)
    squares = lax.psum(jnp.sum(values * values, axis=-1), "tensor")
    scale = lax.rsqrt(squares / width + norm_eps)[:, :, None]
    normed = (values * scale * gain_full).astype(jnp.bfloat16)
    logits = lax.psum(jnp.dot(normed, router, preferred_element_type=jnp.float32), "tensor")
    chosen = routes[0]
    onehot = (chosen[..., None] == expert_ids).astype(jnp.float32)
    picked = jnp.sum(onehot * logits[:, :, None, :], axis=-1)
    delta = picked[..., 0] - picked[..., 1]
    packed = jnp.concatenate([chosen.astype(jnp.float32), delta[..., None]], axis=-1)
    packed = jnp.swapaxes(lax.all_gather(packed, "expert"), 0, 1)
    named = packed[..., :2].astype(jnp.int32)
    q0, q1 = jax.nn.sigmoid(packed[..., 2]), jax.nn.sigmoid(-packed[..., 2])
    is0, is1 = named[..., 0] == own, named[..., 1] == own
    used = jnp.logical_or(is0, is1)
    count = used.astype(jnp.float32)
    earlier = jnp.tril(jnp.ones((T, T), jnp.float32), -1)
    pos = jnp.einsum("mbt,ut->mbu", count, earlier)
    pos = jnp.where(used, pos, -1.0)
    q_own = jnp.where(is0, q0, jnp.where(is1, q1, 0.0))
    q_other = jnp.where(is0, q1, jnp.where(is1, -q0, 0.0))
    sign = (named[..., 0:1] == expert_ids).astype(jnp.float32) - (
        named[..., 1:2] == expert_ids
    ).astype(jnp.float32)
    info = jnp.concatenate([pos[..., None], q_own[..., None], q_other[..., None], sign], axis=-1)
    info = jnp.pad(info, ((0, 0), (0, 0), (0, 0), (0, lanes - info.shape[-1])))
    info = info.reshape(micros, n, n, T, lanes)
    router_all = lax.all_gather(router, "tensor", axis=0, tiled=True)
    rp = jnp.pad(router_all, ((0, 0), (3, lanes - 3 - experts)))
    scale_wide = jnp.broadcast_to(scale, (micros, T, lanes))

    bf, f32 = jnp.bfloat16, jnp.float32
    vm = pl.BlockSpec(memory_space=pltpu.VMEM)
    anym = pl.BlockSpec(memory_space=pl.ANY)
    dma = pltpu.SemaphoreType.DMA
    K = 2 * F + lanes
    grads = pl.pallas_call(
        functools.partial(kernel, sections, n, (micros, T, Q, F, cap, lanes)),
        out_shape=jax.ShapeDtypeStruct((micros, T, Q), bf),
        in_specs=[vm] * 4 + [anym] * 7,
        out_specs=vm,
        scratch_shapes=[
            pltpu.VMEM((2, n, n, 2, T, Q), bf),
            pltpu.VMEM((2, n, n, 2, T, Q), bf),
            pltpu.VMEM((n, n, 2, T, Q), bf),
            pltpu.VMEM((2, n, T, Q), bf),
            pltpu.VMEM((2, n, 2, T, Q), bf),
            pltpu.VMEM((2, T, Q), bf),
            pltpu.VMEM((2, 2, T, Q), bf),
            pltpu.VMEM((T, Q), bf),
            pltpu.VMEM((micros, T, Q), bf),
            pltpu.VMEM((3, T, lanes), f32),
            pltpu.VMEM((T, lanes), f32),
            pltpu.VMEM((n, n, T, F), f32),
            pltpu.VMEM((n, n, T, F), f32),
            pltpu.VMEM((n, n, T, F), f32),
            pltpu.VMEM((n, n, T, F), bf),
            pltpu.VMEM((n, n, T, K), bf),
            pltpu.VMEM((F, width), bf),
            pltpu.VMEM((width, K), bf),
            pltpu.VMEM((n, n, T, lanes), f32),
            pltpu.VMEM((n * n, cap, F), bf),
            pltpu.VMEM((n * n, cap, F), bf),
            dma((7,)),
            dma, dma,
            dma((2, 2)), dma((2, 2)), dma((2,)), dma((2,)),
            dma((4, 2)), dma((4, 2)), dma((4, 2)), dma((4, 2)),
            dma((4, 4)), dma((4, 4)),
            dma((4,)), dma((4,)), dma((2,)), dma((2,)), dma((2, 4)), dma((2, 4)),
            dma((2,)), dma((2,)), dma((2,)), dma((2,)), dma, dma,
            dma((3,)), dma((3,)), dma((micros,)), dma((micros,)),
            pltpu.SemaphoreType.REGULAR,
        ],
        compiler_params=pltpu.CompilerParams(
            collective_id=0, has_side_effects=True, vmem_limit_bytes=66_000_000
        ),
        name="layer_back",
    )(
        grad_out, layer_inputs[0], scale_wide, gain_full, info, saved_gate[0], saved_up[0],
        w_down[0], w_gate[0], w_up[0], rp,
    )
    return grads[None]


def solution(mesh):
    placed = (
        P("section", None, "expert", "tensor"),
        P(None, "expert", "tensor"),
        P("section", "tensor"),
        P("section", "tensor", None),
        P("section", None, ("expert", "tensor")),
        P("section", None, ("expert", "tensor")),
        P("section", ("expert", "tensor"), None),
        P("section", None, None, None, ("expert", "tensor")),
        P("section", None, None, None, ("expert", "tensor")),
        P("section", None, "expert", None),
    )
    return jax.shard_map(
        on_device,
        mesh=mesh,
        in_specs=placed,
        out_specs=P("section", None, "expert", "tensor"),
        check_vma=False,
    )
```

```python
import functools
import jax
import jax.numpy as jnp
from jax import lax
from jax.experimental import pallas as pl
from jax.experimental.pallas import tpu as pltpu
from jax.sharding import PartitionSpec as P

norm_eps = 1e-05
OFF = (0, -1, 1, 2)
MESH = pl.DeviceIdType.MESH
NT = (((1,), (1,)), ((), ()))


def kernel(
    sections, n, sizes,
    gout, xin, gain, rt_in, rows_in, sg_h, su_h, wd_h, wg_h, wu_h, rp_h,
    out,
    G, U, D, RH, RF, RHF, RFF, RX, hop, mrecv, msend,
    V, A, B, bt, DC, wd, wc, info, sg, su,
    xo, gain_o, ps, pr, tot, GI, tmp,
    ld, x_s, x_r, fo_s, fo_r, ff_s, ff_r, so_s, so_r, sf_s, sf_r, dd_s, dd_r,
    e_s, e_r, rh_s, rh_r, rf_s, rf_r, hf_s, hf_r, ff2_s, ff2_r, rx_s, rx_r,
    m_s, m_r, hop_s, hop_r, xo_s, xo_r, go_s, go_r, rp_s, rp_r, ps_s, ps_r, y_s, y_r, z_s, z_r, gate,
):
    micros, T, Q, F, cap, lanes = sizes
    width = 4 * Q
    K = 2 * F + lanes
    sec = lax.axis_index("section")
    ex = lax.axis_index("expert")
    te = lax.axis_index("tensor")
    z, y = ex // n, ex % n
    xl, c = te // 2, te % 2
    fp = y * (1 - c) + z * c
    sp = z * (1 - c) + y * c

    def at(v, o):
        return lax.rem(v + o + n, n)

    def exid(f, s):
        return (1 - c) * (s * n + f) + c * (f * n + s)

    partner = {"tensor": xl * 2 + 1 - c}
    xnbr = {"tensor": (1 - xl) * 2 + c}
    xdiag = {"tensor": (1 - xl) * 2 + 1 - c}
    fdir = ({"expert": exid(at(fp, 1), sp)}, {"expert": exid(at(fp, -1), sp)})
    sdir = ({"expert": exid(fp, at(sp, 1))}, {"expert": exid(fp, at(sp, -1))})
    across = (partner, xnbr, xdiag)
    ypeer = tuple({"expert": z * n + at(y, o)} for o in (1, 2, 3))
    zpeer = tuple({"expert": at(z, o) * n + y} for o in (1, 2, 3))
    hoppeer = {"section": 1 - sec, "tensor": (1 - xl) * 2 + c}
    near = across + fdir + sdir

    def load(k, src, dst):
        return pltpu.make_async_copy(src, dst, ld.at[k])

    def weight_loads():
        return (
            load(0, wd_h, wd),
            load(1, wg_h, wc.at[:, pl.ds(0, F)]),
            load(2, wu_h, wc.at[:, pl.ds(F, F)]),
            load(3, rp_h, wc.at[pl.ds(pl.multiple_of(te * Q, Q), Q), pl.ds(2 * F, lanes)]),
        )

    for cp in weight_loads():
        cp.start()

    barrier = pltpu.get_barrier_semaphore()
    greeted = across + ypeer + zpeer + ((hoppeer,) if sections == 2 else ())
    for peer in greeted:
        pl.semaphore_signal(barrier, inc=1, device_id=peer, device_id_type=MESH)
    pl.semaphore_wait(barrier, len(greeted))

    def rc(src, dst, ss, rs, peer):
        return pltpu.make_async_remote_copy(
            src_ref=src, dst_ref=dst, send_sem=ss, recv_sem=rs, device_id=peer, device_id_type=MESH
        )

    def send(src, dst, ss, rs, peer):
        rc(src, dst, ss, rs, peer).start()

    def arrived(ref, ss, rs, peer):
        rc(ref, ref, ss, rs, peer).wait_recv()

    def tensor_parts():
        ps[...] = jnp.zeros_like(ps)
        gr = rt_in[...].astype(jnp.float32) * gain[...]
        hi = gr.astype(jnp.bfloat16)
        lo = (gr - hi.astype(jnp.float32)).astype(jnp.bfloat16)
        ones = jnp.ones((16, Q), jnp.bfloat16)
        row = lax.broadcasted_iota(jnp.int32, (8, T), 0)

        def nt(a, b):
            return lax.dot_general(a, b, NT, preferred_element_type=jnp.float32)

        for m in range(micros):
            x = xin[m]
            sq = x.astype(jnp.float32) * x.astype(jnp.float32)
            h = sq.astype(jnp.bfloat16)
            low = (sq - h.astype(jnp.float32)).astype(jnp.bfloat16)
            logit = nt(hi, x) + nt(lo, x)
            total = nt(ones, h) + nt(ones, low)
            ps[m, :, 0:T] = jnp.where(row == 4, total[0:8], logit[0:8])
        for i, peer in enumerate(across):
            send(ps, pr.at[i], ps_s.at[i], ps_r.at[i], peer)

    def spread_inputs():
        send(xin, xo, xo_s, xo_r, xnbr)
        send(gain, gain_o, go_s, go_r, xnbr)
        for i, peer in enumerate(across):
            place = wc.at[pl.ds(pl.multiple_of(te * Q, Q), Q), pl.ds(2 * F, lanes)]
            send(rp_h, place, rp_s.at[i], rp_r.at[i], peer)

    def route_rows():
        for i, peer in enumerate(across):
            arrived(pr.at[i], ps_s.at[i], ps_r.at[i], peer)
        for m in range(micros):
            tot[m] = (ps[m] + pr[0, m]) + (pr[1, m] + pr[2, m])
            sc = lax.rsqrt(tot[m, 4:5] / width + norm_eps)
            e0, e1 = rows_in[m, 0:1], rows_in[m, 1:2]
            delta = jnp.zeros_like(sc)
            for k in range(4):
                pick = jnp.where(e0 == k, 1.0, 0.0) - jnp.where(e1 == k, 1.0, 0.0)
                delta = delta + pick * (tot[m, k : k + 1] * sc)
            GI[z, y, m, 0:1] = e0
            GI[z, y, m, 1:2] = e1
            GI[z, y, m, 2:3] = delta
            GI[z, y, m, 3:4] = sc
        for i, peer in enumerate(ypeer):
            send(GI.at[z, y], GI.at[z, y], y_s.at[i], y_r.at[i], peer)

    def rows_along_y():
        for i in range(3):
            arrived(GI.at[z, at(y, -1 - i)], y_s.at[i], y_r.at[i], ypeer[i])
        for i, peer in enumerate(zpeer):
            send(GI.at[z], GI.at[z], z_s.at[i], z_r.at[i], peer)

    def rows_along_z():
        for i in range(3):
            arrived(GI.at[at(z, -1 - i)], z_s.at[i], z_r.at[i], zpeer[i])
        own = z.astype(jnp.float32)
        before = lax.broadcasted_iota(jnp.int32, (lanes, lanes), 0) < lax.broadcasted_iota(
            jnp.int32, (lanes, lanes), 1
        )
        before = jnp.where(before, 1.0, 0.0).astype(jnp.bfloat16)
        for m in range(micros):
            for j in range(n * n):
                for r in range(4):
                    tmp[r, j : j + 1] = GI[j // n, j % n, m, r : r + 1]
            e0, e1, delta = tmp[0], tmp[1], tmp[2]
            is0 = jnp.where(e0 == own, 1.0, 0.0)
            is1 = jnp.where(e1 == own, 1.0, 0.0)
            used = is0 + is1
            pos = jnp.dot(used.astype(jnp.bfloat16), before, preferred_element_type=jnp.float32)
            pos = jnp.where(used > 0.5, pos, -1.0)
            q0, q1 = jax.nn.sigmoid(delta), jax.nn.sigmoid(-delta)
            parts = [pos, is0 * q0 + is1 * q1, is0 * q1 - is1 * q0]
            for k in range(4):
                parts.append(jnp.where(e0 == k, 1.0, 0.0) - jnp.where(e1 == k, 1.0, 0.0))
            parts.append(tmp[3])
            turned = jnp.concatenate(parts, axis=0).T[0:T]
            for j in range(n * n):
                info[m, j // n, j % n] = pltpu.roll(turned, (lanes - j) % lanes, 1)

    def finish_prologue():
        arrived(xo, xo_s, xo_r, xnbr)
        arrived(gain_o, go_s, go_r, xnbr)
        for i, o in enumerate((xl * 2 + 1 - c, (1 - xl) * 2 + c, (1 - xl) * 2 + 1 - c)):
            place = wc.at[pl.ds(pl.multiple_of(o * Q, Q), Q), pl.ds(2 * F, lanes)]
            arrived(place, rp_s.at[i], rp_r.at[i], across[i])
        rc(xin, xo, xo_s, xo_r, xnbr).wait_send()
        rc(gain, gain_o, go_s, go_r, xnbr).wait_send()
        for i, peer in enumerate(across):
            place = wc.at[pl.ds(pl.multiple_of(te * Q, Q), Q), pl.ds(2 * F, lanes)]
            rc(rp_h, place, rp_s.at[i], rp_r.at[i], peer).wait_send()
            rc(ps, pr.at[i], ps_s.at[i], ps_r.at[i], peer).wait_send()
        for i, peer in enumerate(ypeer):
            rc(GI.at[z, y], GI.at[z, y], y_s.at[i], y_r.at[i], peer).wait_send()
        for i, peer in enumerate(zpeer):
            rc(GI.at[z], GI.at[z], z_s.at[i], z_r.at[i], peer).wait_send()

    def one_micro(m, carry):
        def first(f):
            pl.when(m == 0)(f)

        @pl.when(m > 0)
        def _():
            for peer in near:
                pl.semaphore_signal(gate, inc=1, device_id=peer, device_id_type=MESH)
            pl.semaphore_wait(gate, len(near))

        small = (
            load(4, sg_h.at[m], sg),
            load(5, su_h.at[m], su),
        )
        for cp in small:
            cp.start()
        sent = []

        def go(*a):
            cp = rc(*a)
            cp.start()
            sent.append(cp)

        def got(ref, ss, rs, peer):
            rc(ref, ref, ss, rs, peer).wait_recv()

        top = sec == sections - 1
        qh = jnp.where(top, xl, 1 - xl)
        qo = 1 - qh
        mine = G.at[c, sp, fp]

        @pl.when(top)
        def _():
            G[c, sp, fp, qh] = gout[m]

        if sections == 2:

            @pl.when(jnp.logical_not(top))
            def _():
                got(hop.at[m], hop_s.at[m], hop_r.at[m], hoppeer)
                G[c, sp, fp, qh] = hop[m]

        go(mine.at[qh], mine.at[qh], x_s, x_r, xnbr)
        for d in range(2):
            go(mine.at[qh], mine.at[qh], fo_s.at[0, d], fo_r.at[0, d], fdir[d])
        first(tensor_parts)
        V[...] = jnp.zeros_like(V)
        got(mine.at[qo], x_s, x_r, xnbr)
        for d in range(2):
            go(mine.at[qo], mine.at[qo], fo_s.at[1, d], fo_r.at[1, d], fdir[d])

        def spread(k, slot):
            for d in range(2):
                go(slot, slot, so_s.at[k, d], so_r.at[k, d], sdir[d])

        def share(kk, k, slot):
            go(slot, slot, dd_s.at[kk, k], dd_r.at[kk, k], partner)

        spread(0, mine)
        share(0, 0, mine)
        first(spread_inputs)
        first(route_rows)
        for cp in small:
            cp.wait()

        @first
        def _():
            for cp in weight_loads():
                cp.wait()

        def prepare(j, carry):
            i0, i1 = j // n, j % n
            pos = info[m, i0, i1, :, 0:1]
            slots = lax.broadcasted_iota(jnp.int32, (T, cap), 1).astype(jnp.float32)
            place = jnp.where(slots == pos, 1.0, 0.0).astype(jnp.bfloat16)
            a = jnp.dot(place, sg[j], preferred_element_type=jnp.float32)
            b = jnp.dot(place, su[j], preferred_element_type=jnp.float32)
            sig = jax.nn.sigmoid(a)
            A[i0, i1] = b * sig * (1.0 + a * (1.0 - sig))
            B[i0, i1] = a * sig
            bt[i0, i1] = b.astype(jnp.bfloat16)
            return carry

        def prepare_rows(i):
            lax.fori_loop(i * n, (i + 1) * n, prepare, 0)

        def into_v(kk):
            for k in range(n):
                ref = G.at[1 - c, at(fp, OFF[kk]), at(sp, OFF[k])]
                got(ref, dd_s.at[kk, k], dd_r.at[kk, k], partner)
            zi, yi = at(z, OFF[kk]), at(y, OFF[kk])
            for h in range(2):
                part = jnp.zeros((n * T, F), jnp.float32)
                for q in range(2):
                    g = (G[0, zi, :, q] if h == 0 else G[1, yi, :, q]).reshape(n * T, Q)
                    w = wd[:, (2 * q + h) * Q : (2 * q + h + 1) * Q]
                    part = part + lax.dot_general(g, w, NT, preferred_element_type=jnp.float32)
                part = part.reshape(n, T, F)
                if h == 0:
                    V[zi] += part
                else:
                    V[:, yi] += part

        for d in range(2):
            f = at(fp, -1 if d == 0 else 1)
            slot = G.at[c, sp, f]
            for i, q in enumerate((qh, qo)):
                got(slot.at[q], fo_s.at[i, d], fo_r.at[i, d], fdir[d])
            go(slot.at[d], slot.at[d], ff_s.at[d], ff_r.at[d], fdir[d])
            spread(1 + d, slot)
            share(0, 1 + d, slot)
        first(rows_along_y)
        far = G.at[c, sp, at(fp, 2)]
        for d in range(2):
            got(far.at[d], ff_s.at[d], ff_r.at[d], fdir[d])
        spread(3, far)
        share(0, 3, far)

        def pass_on(k):
            f = at(fp, OFF[k])
            for d in range(2):
                slot = G.at[c, at(sp, -1 if d == 0 else 1), f]
                got(slot, so_s.at[k, d], so_r.at[k, d], sdir[d])
                go(slot.at[d], slot.at[d], sf_s.at[k, d], sf_r.at[k, d], sdir[d])
                share(1 + d, k, slot)

        first(rows_along_z)
        pass_on(0)
        prepare_rows(0)
        pass_on(1)
        into_v(0)
        prepare_rows(1)
        pass_on(2)
        prepare_rows(2)
        pass_on(3)
        prepare_rows(3)
        first(finish_prologue)
        for k in range(n):
            slot = G.at[c, at(sp, 2), at(fp, OFF[k])]
            for d in range(2):
                got(slot.at[d], sf_s.at[k, d], sf_r.at[k, d], sdir[d])
            share(3, k, slot)
            if k == 1:
                into_v(1)
            if k == 2:
                into_v(2)
        into_v(3)

        def finish(j, carry):
            i0, i1 = j // n, j % n
            v = V[i0, i1]
            db = v * B[i0, i1]
            w = jnp.sum(db * bt[i0, i1].astype(jnp.float32), axis=-1, keepdims=True)
            row = info[m, i0, i1]
            DC[i0, i1, :, 0:F] = (v * A[i0, i1]).astype(jnp.bfloat16)
            DC[i0, i1, :, F : 2 * F] = db.astype(jnp.bfloat16)
            DC[i0, i1, :, 2 * F :] = (w * row[:, 32:33] * row).astype(jnp.bfloat16)
            return carry

        lax.fori_loop(0, n * n, finish, 0)

        def into_u(kk):
            zi, yi = at(z, OFF[kk]), at(y, OFF[kk])
            for h in range(2):
                da = (DC[zi] if h == 0 else DC[:, yi]).reshape(n * T, K)
                q_own = (info[m, zi, :, :, 16:17] if h == 0 else info[m, :, yi, :, 16:17]).reshape(n * T, 1)

                def half(q, carry):
                    low = pl.multiple_of((2 * q + h) * Q, Q)
                    u = lax.dot_general(
                        da, wc[pl.ds(low, Q), :], NT, preferred_element_type=jnp.float32
                    )
                    u = (u * q_own).astype(jnp.bfloat16).reshape(n, T, Q)
                    U[h, zi if h == 0 else yi, :, q] = u
                    return carry

                lax.fori_loop(0, 2, half, 0)
            go(U.at[1 - c, at(fp, OFF[kk])], D.at[kk], e_s.at[kk], e_r.at[kk], partner)

        def add_partner(kk):
            got(D.at[kk], e_s.at[kk], e_r.at[kk], partner)
            i = at(sp, OFF[kk])
            U[c, i] = U[c, i] + D[kk]

        into_u(3)
        add_partner(3)
        s2 = at(sp, 2)
        for d in range(2):
            go(U.at[c, s2, :, d], RH.at[d], rh_s.at[d], rh_r.at[d], sdir[d])
        into_u(2)
        add_partner(2)
        into_u(1)
        add_partner(1)
        for d in range(2):
            i = at(sp, 1 if d == 0 else -1)
            got(RH.at[d], rh_s.at[d], rh_r.at[d], sdir[d])
            U[c, i, :, d] = U[c, i, :, d] + RH[d]
            for k in (3, 2, 1, 0):
                f = at(fp, OFF[k])
                go(U.at[c, i, f], RF.at[d, k], rf_s.at[d, k], rf_r.at[d, k], sdir[d])
        into_u(0)
        add_partner(0)

        def own_sum(k):
            for d in range(2):
                got(RF.at[d, k], rf_s.at[d, k], rf_r.at[d, k], sdir[d])
            f = at(fp, OFF[k])
            total = U[c, sp, f].astype(jnp.float32) + RF[0, k].astype(jnp.float32)
            U[c, sp, f] = (total + RF[1, k].astype(jnp.float32)).astype(jnp.bfloat16)

        own_sum(3)
        f2 = at(fp, 2)
        for d in range(2):
            go(U.at[c, sp, f2, d], RHF.at[d], hf_s.at[d], hf_r.at[d], fdir[d])
        for d, k in ((0, 2), (1, 1)):
            own_sum(k)
            f = at(fp, OFF[k])
            got(RHF.at[d], hf_s.at[d], hf_r.at[d], fdir[d])
            U[c, sp, f, d] = U[c, sp, f, d] + RHF[d]
            go(U.at[c, sp, f], RFF.at[d], ff2_s.at[d], ff2_r.at[d], fdir[d])
        own_sum(0)
        for d in range(2):
            got(RFF.at[d], ff2_s.at[d], ff2_r.at[d], fdir[d])

        def three(q):
            total = U[c, sp, fp, q].astype(jnp.float32) + RFF[0, q].astype(jnp.float32)
            return total + RFF[1, q].astype(jnp.float32)

        other = three(1 - xl)
        U[c, sp, fp, 1 - xl] = other.astype(jnp.bfloat16)
        go(U.at[c, sp, fp, 1 - xl], RX, rx_s, rx_r, xnbr)
        dn = three(xl)

        values = xin[m].astype(jnp.float32)
        both = values * (dn * gain[...]) + xo[m].astype(jnp.float32) * (other * gain_o[...])
        msend[...] = jnp.broadcast_to(jnp.sum(both, axis=-1, keepdims=True), msend.shape)
        for i, peer in enumerate(across):
            go(msend, mrecv.at[i], m_s.at[i], m_r.at[i], peer)
        got(RX, rx_s, rx_r, xnbr)
        gained = (dn + RX[...].astype(jnp.float32)) * gain[...]
        for i, peer in enumerate(across):
            got(mrecv.at[i], m_s.at[i], m_r.at[i], peer)
        moment = (msend[...] + mrecv[0] + mrecv[1] + mrecv[2])[:, 0:1] / width
        sc = info[m, z, y, :, 112:113]
        result = G[c, sp, fp, xl].astype(jnp.float32) + sc * gained - values * (sc * sc * sc * moment)
        out[m] = result.astype(jnp.bfloat16)
        if sections == 2:

            @pl.when(top)
            def _():
                rc(out.at[m], hop.at[m], hop_s.at[m], hop_r.at[m], hoppeer).start()

        for cp in sent:
            cp.wait_send()
        if sections == 2:

            @pl.when(top)
            def _():
                rc(out.at[m], hop.at[m], hop_s.at[m], hop_r.at[m], hoppeer).wait_send()

        return carry

    lax.fori_loop(0, micros, one_micro, 0)


def on_device(
    layer_inputs, grad_out, norm_gain, router_w, w_gate, w_up, w_down, saved_gate, saved_up, routes
):
    sections = lax.axis_size("section")
    n = 4
    micros, T, Q = grad_out.shape
    F = w_gate.shape[2]
    cap = saved_gate.shape[3]
    lanes = 128
    router = router_w[0]
    experts = router.shape[1]
    width = w_gate.shape[1]
    gain_full = norm_gain.astype(jnp.float32)
    turned = jnp.pad(router.T, ((0, 16 - experts), (0, 0)))
    rows = jnp.swapaxes(routes[0], 1, 2).astype(jnp.float32)
    rows = jnp.pad(rows, ((0, 0), (0, 6), (0, lanes - T)), constant_values=-5.0)
    spaced = jnp.pad(router[:, :, None], ((0, 0), (0, 0), (0, 15))).reshape(Q, experts * 16)
    rp = jnp.pad(spaced, ((0, 0), (48, lanes - 48 - experts * 16)))

    bf, f32 = jnp.bfloat16, jnp.float32
    vm = pl.BlockSpec(memory_space=pltpu.VMEM)
    anym = pl.BlockSpec(memory_space=pl.ANY)
    dma = pltpu.SemaphoreType.DMA
    K = 2 * F + lanes
    grads = pl.pallas_call(
        functools.partial(kernel, sections, n, (micros, T, Q, F, cap, lanes)),
        out_shape=jax.ShapeDtypeStruct((micros, T, Q), bf),
        in_specs=[vm] * 5 + [anym] * 6,
        out_specs=vm,
        scratch_shapes=[
            pltpu.VMEM((2, n, n, 2, T, Q), bf),
            pltpu.VMEM((2, n, n, 2, T, Q), bf),
            pltpu.VMEM((n, n, 2, T, Q), bf),
            pltpu.VMEM((2, n, T, Q), bf),
            pltpu.VMEM((2, n, 2, T, Q), bf),
            pltpu.VMEM((2, T, Q), bf),
            pltpu.VMEM((2, 2, T, Q), bf),
            pltpu.VMEM((T, Q), bf),
            pltpu.VMEM((micros, T, Q), bf),
            pltpu.VMEM((3, T, lanes), f32),
            pltpu.VMEM((T, lanes), f32),
            pltpu.VMEM((n, n, T, F), f32),
            pltpu.VMEM((n, n, T, F), f32),
            pltpu.VMEM((n, n, T, F), f32),
            pltpu.VMEM((n, n, T, F), bf),
            pltpu.VMEM((n, n, T, K), bf),
            pltpu.VMEM((F, width), bf),
            pltpu.VMEM((width, K), bf),
            pltpu.VMEM((micros, n, n, T, lanes), f32),
            pltpu.VMEM((n * n, cap, F), bf),
            pltpu.VMEM((n * n, cap, F), bf),
            pltpu.VMEM((micros, T, Q), bf),
            pltpu.VMEM((1, Q), f32),
            pltpu.VMEM((micros, 8, lanes), f32),
            pltpu.VMEM((3, micros, 8, lanes), f32),
            pltpu.VMEM((micros, 8, lanes), f32),
            pltpu.VMEM((n, n, micros, 8, lanes), f32),
            pltpu.VMEM((4, n * n, lanes), f32),
            dma((6,)),
            dma, dma,
            dma((2, 2)), dma((2, 2)), dma((2,)), dma((2,)),
            dma((4, 2)), dma((4, 2)), dma((4, 2)), dma((4, 2)),
            dma((4, 4)), dma((4, 4)),
            dma((4,)), dma((4,)), dma((2,)), dma((2,)), dma((2, 4)), dma((2, 4)),
            dma((2,)), dma((2,)), dma((2,)), dma((2,)), dma, dma,
            dma((3,)), dma((3,)), dma((micros,)), dma((micros,)),
            dma, dma, dma, dma, dma((3,)), dma((3,)), dma((3,)), dma((3,)),
            dma((3,)), dma((3,)), dma((3,)), dma((3,)),
            pltpu.SemaphoreType.REGULAR,
        ],
        compiler_params=pltpu.CompilerParams(
            collective_id=0, has_side_effects=True, vmem_limit_bytes=66_000_000
        ),
        name="layer_back",
    )(
        grad_out, layer_inputs[0], gain_full, turned, rows, saved_gate[0], saved_up[0],
        w_down[0], w_gate[0], w_up[0], rp,
    )
    return grads[None]


def solution(mesh):
    placed = (
        P("section", None, "expert", "tensor"),
        P(None, "expert", "tensor"),
        P("section", "tensor"),
        P("section", "tensor", None),
        P("section", None, ("expert", "tensor")),
        P("section", None, ("expert", "tensor")),
        P("section", ("expert", "tensor"), None),
        P("section", None, None, None, ("expert", "tensor")),
        P("section", None, None, None, ("expert", "tensor")),
        P("section", None, "expert", None),
    )
    return jax.shard_map(
        on_device,
        mesh=mesh,
        in_specs=placed,
        out_specs=P("section", None, "expert", "tensor"),
        check_vma=False,
    )
```

```python
import functools
import jax
import jax.numpy as jnp
from jax import lax
from jax.experimental import pallas as pl
from jax.experimental.pallas import tpu as pltpu
from jax.sharding import PartitionSpec as P

norm_eps = 1e-05
OFF = (0, -1, 1, 2)
MESH = pl.DeviceIdType.MESH
NT = (((1,), (1,)), ((), ()))


def kernel(
    sections, n, sizes,
    gout, xin, gain, rt_in, rows_in, sg_h, su_h, wd_h, wg_h, wu_h, rp_h,
    out,
    G, U, D, RH, RF, RHF, RFF, RX, hop, mrecv, msend,
    V, A, B, bt, DC, wd, wc, info, sg, su,
    xo, gain_o, ps, pr, tot, GI, tmp,
    ld, x_s, x_r, fo_s, fo_r, ff_s, ff_r, sq_s, sq_r, so_s, so_r, sf_s, sf_r, dd_s, dd_r,
    e_s, e_r, rh_s, rh_r, rf_s, rf_r, hf_s, hf_r, ff2_s, ff2_r, rx_s, rx_r,
    m_s, m_r, hop_s, hop_r, xo_s, xo_r, go_s, go_r, rp_s, rp_r, ps_s, ps_r, y_s, y_r, z_s, z_r, gate,
):
    micros, T, Q, F, cap, lanes = sizes
    width = 4 * Q
    K = 2 * F + lanes
    sec = lax.axis_index("section")
    ex = lax.axis_index("expert")
    te = lax.axis_index("tensor")
    z, y = ex // n, ex % n
    xl, c = te // 2, te % 2
    fp = y * (1 - c) + z * c
    sp = z * (1 - c) + y * c

    def at(v, o):
        return lax.rem(v + o + n, n)

    def exid(f, s):
        return (1 - c) * (s * n + f) + c * (f * n + s)

    partner = {"tensor": xl * 2 + 1 - c}
    xnbr = {"tensor": (1 - xl) * 2 + c}
    xdiag = {"tensor": (1 - xl) * 2 + 1 - c}
    fdir = ({"expert": exid(at(fp, 1), sp)}, {"expert": exid(at(fp, -1), sp)})
    sdir = ({"expert": exid(fp, at(sp, 1))}, {"expert": exid(fp, at(sp, -1))})
    across = (partner, xnbr, xdiag)
    ypeer = tuple({"expert": z * n + at(y, o)} for o in (1, 2, 3))
    zpeer = tuple({"expert": at(z, o) * n + y} for o in (1, 2, 3))
    hoppeer = {"section": 1 - sec, "tensor": (1 - xl) * 2 + c}
    near = across + fdir + sdir

    def load(k, src, dst):
        return pltpu.make_async_copy(src, dst, ld.at[k])

    def weight_loads():
        return (
            load(0, wd_h, wd),
            load(1, wg_h, wc.at[:, pl.ds(0, F)]),
            load(2, wu_h, wc.at[:, pl.ds(F, F)]),
            load(3, rp_h, wc.at[pl.ds(pl.multiple_of(te * Q, Q), Q), pl.ds(2 * F, lanes)]),
        )

    for cp in weight_loads():
        cp.start()

    barrier = pltpu.get_barrier_semaphore()
    greeted = across + ypeer + zpeer + ((hoppeer,) if sections == 2 else ())
    for peer in greeted:
        pl.semaphore_signal(barrier, inc=1, device_id=peer, device_id_type=MESH)
    pl.semaphore_wait(barrier, len(greeted))

    def rc(src, dst, ss, rs, peer):
        return pltpu.make_async_remote_copy(
            src_ref=src, dst_ref=dst, send_sem=ss, recv_sem=rs, device_id=peer, device_id_type=MESH
        )

    def send(src, dst, ss, rs, peer):
        rc(src, dst, ss, rs, peer).start()

    def arrived(ref, ss, rs, peer):
        rc(ref, ref, ss, rs, peer).wait_recv()

    def tensor_parts():
        ps[...] = jnp.zeros_like(ps)
        gr = rt_in[...].astype(jnp.float32) * gain[...]
        hi = gr.astype(jnp.bfloat16)
        lo = (gr - hi.astype(jnp.float32)).astype(jnp.bfloat16)
        ones = jnp.ones((16, Q), jnp.bfloat16)
        row = lax.broadcasted_iota(jnp.int32, (8, T), 0)

        def nt(a, b):
            return lax.dot_general(a, b, NT, preferred_element_type=jnp.float32)

        for m in range(micros):
            x = xin[m]
            sq = x.astype(jnp.float32) * x.astype(jnp.float32)
            h = sq.astype(jnp.bfloat16)
            low = (sq - h.astype(jnp.float32)).astype(jnp.bfloat16)
            logit = nt(hi, x) + nt(lo, x)
            total = nt(ones, h) + nt(ones, low)
            ps[m, :, 0:T] = jnp.where(row == 4, total[0:8], logit[0:8])
        for i, peer in enumerate(across):
            send(ps, pr.at[i], ps_s.at[i], ps_r.at[i], peer)

    def spread_inputs():
        send(xin, xo, xo_s, xo_r, xnbr)
        send(gain, gain_o, go_s, go_r, xnbr)
        for i, peer in enumerate(across):
            place = wc.at[pl.ds(pl.multiple_of(te * Q, Q), Q), pl.ds(2 * F, lanes)]
            send(rp_h, place, rp_s.at[i], rp_r.at[i], peer)

    def route_rows():
        for i, peer in enumerate(across):
            arrived(pr.at[i], ps_s.at[i], ps_r.at[i], peer)
        for m in range(micros):
            tot[m] = (ps[m] + pr[0, m]) + (pr[1, m] + pr[2, m])
            sc = lax.rsqrt(tot[m, 4:5] / width + norm_eps)
            e0, e1 = rows_in[m, 0:1], rows_in[m, 1:2]
            delta = jnp.zeros_like(sc)
            for k in range(4):
                pick = jnp.where(e0 == k, 1.0, 0.0) - jnp.where(e1 == k, 1.0, 0.0)
                delta = delta + pick * (tot[m, k : k + 1] * sc)
            GI[z, y, m, 0:1] = e0
            GI[z, y, m, 1:2] = e1
            GI[z, y, m, 2:3] = delta
            GI[z, y, m, 3:4] = sc
        for i, peer in enumerate(ypeer):
            send(GI.at[z, y], GI.at[z, y], y_s.at[i], y_r.at[i], peer)

    def rows_along_y():
        for i in range(3):
            arrived(GI.at[z, at(y, -1 - i)], y_s.at[i], y_r.at[i], ypeer[i])
        for i, peer in enumerate(zpeer):
            send(GI.at[z], GI.at[z], z_s.at[i], z_r.at[i], peer)

    def rows_along_z():
        for i in range(3):
            arrived(GI.at[at(z, -1 - i)], z_s.at[i], z_r.at[i], zpeer[i])
        own = z.astype(jnp.float32)
        before = lax.broadcasted_iota(jnp.int32, (lanes, lanes), 0) < lax.broadcasted_iota(
            jnp.int32, (lanes, lanes), 1
        )
        before = jnp.where(before, 1.0, 0.0).astype(jnp.bfloat16)
        for m in range(micros):
            for j in range(n * n):
                for r in range(4):
                    tmp[r, j : j + 1] = GI[j // n, j % n, m, r : r + 1]
            e0, e1, delta = tmp[0], tmp[1], tmp[2]
            is0 = jnp.where(e0 == own, 1.0, 0.0)
            is1 = jnp.where(e1 == own, 1.0, 0.0)
            used = is0 + is1
            pos = jnp.dot(used.astype(jnp.bfloat16), before, preferred_element_type=jnp.float32)
            pos = jnp.where(used > 0.5, pos, -1.0)
            q0, q1 = jax.nn.sigmoid(delta), jax.nn.sigmoid(-delta)
            parts = [pos, is0 * q0 + is1 * q1, is0 * q1 - is1 * q0]
            for k in range(4):
                parts.append(jnp.where(e0 == k, 1.0, 0.0) - jnp.where(e1 == k, 1.0, 0.0))
            parts.append(tmp[3])
            turned = jnp.concatenate(parts, axis=0).T[0:T]
            for j in range(n * n):
                info[m, j // n, j % n] = pltpu.roll(turned, (lanes - j) % lanes, 1)

    def finish_prologue():
        arrived(xo, xo_s, xo_r, xnbr)
        arrived(gain_o, go_s, go_r, xnbr)
        for i, o in enumerate((xl * 2 + 1 - c, (1 - xl) * 2 + c, (1 - xl) * 2 + 1 - c)):
            place = wc.at[pl.ds(pl.multiple_of(o * Q, Q), Q), pl.ds(2 * F, lanes)]
            arrived(place, rp_s.at[i], rp_r.at[i], across[i])
        rc(xin, xo, xo_s, xo_r, xnbr).wait_send()
        rc(gain, gain_o, go_s, go_r, xnbr).wait_send()
        for i, peer in enumerate(across):
            place = wc.at[pl.ds(pl.multiple_of(te * Q, Q), Q), pl.ds(2 * F, lanes)]
            rc(rp_h, place, rp_s.at[i], rp_r.at[i], peer).wait_send()
            rc(ps, pr.at[i], ps_s.at[i], ps_r.at[i], peer).wait_send()
        for i, peer in enumerate(ypeer):
            rc(GI.at[z, y], GI.at[z, y], y_s.at[i], y_r.at[i], peer).wait_send()
        for i, peer in enumerate(zpeer):
            rc(GI.at[z], GI.at[z], z_s.at[i], z_r.at[i], peer).wait_send()

    def one_micro(m, carry):
        @pl.when(m > 0)
        def _():
            for peer in near:
                pl.semaphore_signal(gate, inc=1, device_id=peer, device_id_type=MESH)
            pl.semaphore_wait(gate, len(near))

        small = (
            load(4, sg_h.at[m], sg),
            load(5, su_h.at[m], su),
        )
        for cp in small:
            cp.start()
        sent = []

        def go(*a):
            cp = rc(*a)
            cp.start()
            sent.append(cp)

        def got(ref, ss, rs, peer):
            rc(ref, ref, ss, rs, peer).wait_recv()

        top = sec == sections - 1
        ahead = jnp.logical_and(m == 0, jnp.logical_not(top))

        def first(f):
            pl.when(jnp.logical_and(m == 0, top))(f)

        def prepare(j, carry):
            i0, i1 = j // n, j % n
            pos = info[m, i0, i1, :, 0:1]
            slots = lax.broadcasted_iota(jnp.int32, (T, cap), 1).astype(jnp.float32)
            place = jnp.where(slots == pos, 1.0, 0.0).astype(jnp.bfloat16)
            a = jnp.dot(place, sg[j], preferred_element_type=jnp.float32)
            b = jnp.dot(place, su[j], preferred_element_type=jnp.float32)
            sig = jax.nn.sigmoid(a)
            A[i0, i1] = b * sig * (1.0 + a * (1.0 - sig))
            B[i0, i1] = a * sig
            bt[i0, i1] = b.astype(jnp.bfloat16)
            return carry

        def prepare_rows(i):
            @pl.when(jnp.logical_not(ahead))
            def _():
                lax.fori_loop(i * n, (i + 1) * n, prepare, 0)

        if sections == 2:

            @pl.when(ahead)
            def _():
                tensor_parts()
                spread_inputs()
                route_rows()
                rows_along_y()
                rows_along_z()
                for cp in small:
                    cp.wait()
                for cp in weight_loads():
                    cp.wait()
                finish_prologue()
                lax.fori_loop(0, n * n, prepare, 0)

        qh = jnp.where(top, xl, 1 - xl)
        qo = 1 - qh
        mine = G.at[c, sp, fp]

        @pl.when(top)
        def _():
            G[c, sp, fp, qh] = gout[m]

        if sections == 2:

            @pl.when(jnp.logical_not(top))
            def _():
                got(hop.at[m], hop_s.at[m], hop_r.at[m], hoppeer)
                G[c, sp, fp, qh] = hop[m]

        go(mine.at[qh], mine.at[qh], x_s, x_r, xnbr)
        for d in range(2):
            go(mine.at[qh], mine.at[qh], fo_s.at[0, d], fo_r.at[0, d], fdir[d])
        for d in range(2):
            go(mine.at[qh], mine.at[qh], sq_s.at[0, d], sq_r.at[0, d], sdir[d])
        first(tensor_parts)
        V[...] = jnp.zeros_like(V)
        got(mine.at[qo], x_s, x_r, xnbr)
        for d in range(2):
            go(mine.at[qo], mine.at[qo], fo_s.at[1, d], fo_r.at[1, d], fdir[d])
        for d in range(2):
            go(mine.at[qo], mine.at[qo], sq_s.at[1, d], sq_r.at[1, d], sdir[d])

        def spread(k, slot):
            for d in range(2):
                go(slot, slot, so_s.at[k, d], so_r.at[k, d], sdir[d])

        def share(kk, k, slot):
            go(slot, slot, dd_s.at[kk, k], dd_r.at[kk, k], partner)

        share(0, 0, mine)
        first(spread_inputs)
        first(route_rows)

        @pl.when(jnp.logical_not(ahead))
        def _():
            for cp in small:
                cp.wait()

        @first
        def _():
            for cp in weight_loads():
                cp.wait()

        def into_v(kk):
            for k in range(n):
                ref = G.at[1 - c, at(fp, OFF[kk]), at(sp, OFF[k])]
                got(ref, dd_s.at[kk, k], dd_r.at[kk, k], partner)
            zi, yi = at(z, OFF[kk]), at(y, OFF[kk])
            for h in range(2):
                part = jnp.zeros((n * T, F), jnp.float32)
                for q in range(2):
                    g = (G[0, zi, :, q] if h == 0 else G[1, yi, :, q]).reshape(n * T, Q)
                    w = wd[:, (2 * q + h) * Q : (2 * q + h + 1) * Q]
                    part = part + lax.dot_general(g, w, NT, preferred_element_type=jnp.float32)
                part = part.reshape(n, T, F)
                if h == 0:
                    V[zi] += part
                else:
                    V[:, yi] += part

        for d in range(2):
            f = at(fp, -1 if d == 0 else 1)
            slot = G.at[c, sp, f]
            for i, q in enumerate((qh, qo)):
                got(slot.at[q], fo_s.at[i, d], fo_r.at[i, d], fdir[d])
            go(slot.at[d], slot.at[d], ff_s.at[d], ff_r.at[d], fdir[d])
            spread(1 + d, slot)
            share(0, 1 + d, slot)
        first(rows_along_y)
        far = G.at[c, sp, at(fp, 2)]
        for d in range(2):
            got(far.at[d], ff_s.at[d], ff_r.at[d], fdir[d])
        spread(3, far)
        share(0, 3, far)

        def pass_on(k):
            f = at(fp, OFF[k])
            for d in range(2):
                slot = G.at[c, at(sp, -1 if d == 0 else 1), f]
                if k == 0:
                    for i, q in enumerate((qh, qo)):
                        got(slot.at[q], sq_s.at[i, d], sq_r.at[i, d], sdir[d])
                else:
                    got(slot, so_s.at[k, d], so_r.at[k, d], sdir[d])
                go(slot.at[d], slot.at[d], sf_s.at[k, d], sf_r.at[k, d], sdir[d])
                share(1 + d, k, slot)

        first(rows_along_z)
        pass_on(0)
        prepare_rows(0)
        pass_on(1)
        into_v(0)
        prepare_rows(1)
        pass_on(2)
        prepare_rows(2)
        pass_on(3)
        prepare_rows(3)
        first(finish_prologue)
        for k in range(n):
            slot = G.at[c, at(sp, 2), at(fp, OFF[k])]
            for d in range(2):
                got(slot.at[d], sf_s.at[k, d], sf_r.at[k, d], sdir[d])
            share(3, k, slot)
            if k == 1:
                into_v(1)
            if k == 2:
                into_v(2)

        def finish(i0, i1):
            v = V[i0, i1]
            db = v * B[i0, i1]
            w = jnp.sum(db * bt[i0, i1].astype(jnp.float32), axis=-1, keepdims=True)
            row = info[m, i0, i1]
            DC[i0, i1, :, 0:F] = (v * A[i0, i1]).astype(jnp.bfloat16)
            DC[i0, i1, :, F : 2 * F] = db.astype(jnp.bfloat16)
            DC[i0, i1, :, 2 * F :] = (w * row[:, 32:33] * row).astype(jnp.bfloat16)

        def finish_near(j, carry):
            i, k = j // 3, j % 3
            finish(at(z, i + i // 2), at(y, k + k // 2))
            return carry

        def finish_far(j, carry):
            k = j - 4
            o = k + k // 2
            finish(at(z, jnp.where(j < 4, 2, o)), at(y, jnp.where(j < 4, j, 2)))
            return carry

        lax.fori_loop(0, 9, finish_near, 0)
        into_v(3)
        lax.fori_loop(0, 7, finish_far, 0)

        def half_u(kk, h, theirs):
            zi, yi = at(z, OFF[kk]), at(y, OFF[kk])
            da = (DC[zi] if h == 0 else DC[:, yi]).reshape(n * T, K)
            q_own = (info[m, zi, :, :, 16:17] if h == 0 else info[m, :, yi, :, 16:17]).reshape(n * T, 1)
            group = zi if h == 0 else yi

            def quarter(q, carry):
                low = pl.multiple_of((2 * q + h) * Q, Q)
                u = lax.dot_general(da, wc[pl.ds(low, Q), :], NT, preferred_element_type=jnp.float32)
                U[h, group, :, q] = (u * q_own).astype(jnp.bfloat16).reshape(n, T, Q)
                if theirs:
                    rc(U.at[h, group, :, q], D.at[kk, :, q], e_s.at[kk, q], e_r.at[kk, q], partner).start()
                return carry

            lax.fori_loop(0, 2, quarter, 0)

        def u_for_partner(kk):
            for core in range(2):
                pl.when(c == core)(functools.partial(half_u, kk, 1 - core, True))
            for q in range(2):
                sent.append(
                    rc(U.at[1 - c, at(fp, OFF[kk]), :, q], D.at[kk, :, q], e_s.at[kk, q], e_r.at[kk, q], partner)
                )

        def u_for_self(kk):
            for core in range(2):
                pl.when(c == core)(functools.partial(half_u, kk, core, False))

        def add_partner(kk, q):
            got(D.at[kk, :, q], e_s.at[kk, q], e_r.at[kk, q], partner)
            i = at(sp, OFF[kk])
            U[c, i, :, q] = U[c, i, :, q] + D[kk, :, q]

        u_for_partner(3)
        u_for_self(3)
        u_for_partner(2)
        s2 = at(sp, 2)
        for d in range(2):
            add_partner(3, d)
            for k in (3, 2, 1, 0):
                go(U.at[c, s2, at(fp, OFF[k]), d], RH.at[d, k], rh_s.at[d, k], rh_r.at[d, k], sdir[d])
        u_for_self(2)
        u_for_partner(1)
        u_for_self(1)
        for q in range(2):
            add_partner(2, q)
        for q in range(2):
            add_partner(1, q)

        def pass_sum(k):
            for d in range(2):
                i, f = at(sp, 1 if d == 0 else -1), at(fp, OFF[k])
                got(RH.at[d, k], rh_s.at[d, k], rh_r.at[d, k], sdir[d])
                U[c, i, f, d] = U[c, i, f, d] + RH[d, k]
                go(U.at[c, i, f], RF.at[d, k], rf_s.at[d, k], rf_r.at[d, k], sdir[d])

        pass_sum(3)
        pass_sum(2)
        u_for_partner(0)
        pass_sum(1)
        pass_sum(0)
        u_for_self(0)
        for q in range(2):
            add_partner(0, q)

        def own_sum(k):
            for d in range(2):
                got(RF.at[d, k], rf_s.at[d, k], rf_r.at[d, k], sdir[d])
            f = at(fp, OFF[k])
            total = U[c, sp, f].astype(jnp.float32) + RF[0, k].astype(jnp.float32)
            U[c, sp, f] = (total + RF[1, k].astype(jnp.float32)).astype(jnp.bfloat16)

        own_sum(3)
        f2 = at(fp, 2)
        for d in range(2):
            go(U.at[c, sp, f2, d], RHF.at[d], hf_s.at[d], hf_r.at[d], fdir[d])
        for d, k in ((0, 2), (1, 1)):
            own_sum(k)
            f = at(fp, OFF[k])
            got(RHF.at[d], hf_s.at[d], hf_r.at[d], fdir[d])
            U[c, sp, f, d] = U[c, sp, f, d] + RHF[d]
            for i, q in enumerate((1 - xl, xl)):
                go(U.at[c, sp, f, q], RFF.at[d, q], ff2_s.at[d, i], ff2_r.at[d, i], fdir[d])
        own_sum(0)

        def three(i, q):
            for d in range(2):
                got(RFF.at[d, q], ff2_s.at[d, i], ff2_r.at[d, i], fdir[d])
            total = U[c, sp, fp, q].astype(jnp.float32) + RFF[0, q].astype(jnp.float32)
            return total + RFF[1, q].astype(jnp.float32)

        other = three(0, 1 - xl)
        U[c, sp, fp, 1 - xl] = other.astype(jnp.bfloat16)
        go(U.at[c, sp, fp, 1 - xl], RX, rx_s, rx_r, xnbr)
        dn = three(1, xl)

        values = xin[m].astype(jnp.float32)
        both = values * (dn * gain[...]) + xo[m].astype(jnp.float32) * (other * gain_o[...])
        msend[...] = jnp.broadcast_to(jnp.sum(both, axis=-1, keepdims=True), msend.shape)
        for i, peer in enumerate(across):
            go(msend, mrecv.at[i], m_s.at[i], m_r.at[i], peer)
        got(RX, rx_s, rx_r, xnbr)
        gained = (dn + RX[...].astype(jnp.float32)) * gain[...]
        for i, peer in enumerate(across):
            got(mrecv.at[i], m_s.at[i], m_r.at[i], peer)
        moment = (msend[...] + mrecv[0] + mrecv[1] + mrecv[2])[:, 0:1] / width
        sc = info[m, z, y, :, 112:113]
        result = G[c, sp, fp, xl].astype(jnp.float32) + sc * gained - values * (sc * sc * sc * moment)
        out[m] = result.astype(jnp.bfloat16)
        if sections == 2:

            @pl.when(top)
            def _():
                rc(out.at[m], hop.at[m], hop_s.at[m], hop_r.at[m], hoppeer).start()

        for cp in sent:
            cp.wait_send()
        if sections == 2:

            @pl.when(top)
            def _():
                rc(out.at[m], hop.at[m], hop_s.at[m], hop_r.at[m], hoppeer).wait_send()

        return carry

    lax.fori_loop(0, micros, one_micro, 0)


def on_device(
    layer_inputs, grad_out, norm_gain, router_w, w_gate, w_up, w_down, saved_gate, saved_up, routes
):
    sections = lax.axis_size("section")
    n = 4
    micros, T, Q = grad_out.shape
    F = w_gate.shape[2]
    cap = saved_gate.shape[3]
    lanes = 128
    router = router_w[0]
    experts = router.shape[1]
    width = w_gate.shape[1]
    gain_full = norm_gain.astype(jnp.float32)
    turned = jnp.pad(router.T, ((0, 16 - experts), (0, 0)))
    rows = jnp.swapaxes(routes[0], 1, 2).astype(jnp.float32)
    rows = jnp.pad(rows, ((0, 0), (0, 6), (0, lanes - T)), constant_values=-5.0)
    spaced = jnp.pad(router[:, :, None], ((0, 0), (0, 0), (0, 15))).reshape(Q, experts * 16)
    rp = jnp.pad(spaced, ((0, 0), (48, lanes - 48 - experts * 16)))

    bf, f32 = jnp.bfloat16, jnp.float32
    vm = pl.BlockSpec(memory_space=pltpu.VMEM)
    anym = pl.BlockSpec(memory_space=pl.ANY)
    dma = pltpu.SemaphoreType.DMA
    K = 2 * F + lanes
    grads = pl.pallas_call(
        functools.partial(kernel, sections, n, (micros, T, Q, F, cap, lanes)),
        out_shape=jax.ShapeDtypeStruct((micros, T, Q), bf),
        in_specs=[vm] * 5 + [anym] * 6,
        out_specs=vm,
        scratch_shapes=[
            pltpu.VMEM((2, n, n, 2, T, Q), bf),
            pltpu.VMEM((2, n, n, 2, T, Q), bf),
            pltpu.VMEM((n, n, 2, T, Q), bf),
            pltpu.VMEM((2, n, T, Q), bf),
            pltpu.VMEM((2, n, 2, T, Q), bf),
            pltpu.VMEM((2, T, Q), bf),
            pltpu.VMEM((2, 2, T, Q), bf),
            pltpu.VMEM((T, Q), bf),
            pltpu.VMEM((micros, T, Q), bf),
            pltpu.VMEM((3, T, lanes), f32),
            pltpu.VMEM((T, lanes), f32),
            pltpu.VMEM((n, n, T, F), f32),
            pltpu.VMEM((n, n, T, F), f32),
            pltpu.VMEM((n, n, T, F), f32),
            pltpu.VMEM((n, n, T, F), bf),
            pltpu.VMEM((n, n, T, K), bf),
            pltpu.VMEM((F, width), bf),
            pltpu.VMEM((width, K), bf),
            pltpu.VMEM((micros, n, n, T, lanes), f32),
            pltpu.VMEM((n * n, cap, F), bf),
            pltpu.VMEM((n * n, cap, F), bf),
            pltpu.VMEM((micros, T, Q), bf),
            pltpu.VMEM((1, Q), f32),
            pltpu.VMEM((micros, 8, lanes), f32),
            pltpu.VMEM((3, micros, 8, lanes), f32),
            pltpu.VMEM((micros, 8, lanes), f32),
            pltpu.VMEM((n, n, micros, 8, lanes), f32),
            pltpu.VMEM((4, n * n, lanes), f32),
            dma((6,)),
            dma, dma,
            dma((2, 2)), dma((2, 2)), dma((2,)), dma((2,)),
            dma((2, 2)), dma((2, 2)), dma((4, 2)), dma((4, 2)), dma((4, 2)), dma((4, 2)),
            dma((4, 4)), dma((4, 4)),
            dma((4, 2)), dma((4, 2)), dma((2, 4)), dma((2, 4)), dma((2, 4)), dma((2, 4)),
            dma((2,)), dma((2,)), dma((2, 2)), dma((2, 2)), dma, dma,
            dma((3,)), dma((3,)), dma((micros,)), dma((micros,)),
            dma, dma, dma, dma, dma((3,)), dma((3,)), dma((3,)), dma((3,)),
            dma((3,)), dma((3,)), dma((3,)), dma((3,)),
            pltpu.SemaphoreType.REGULAR,
        ],
        compiler_params=pltpu.CompilerParams(
            collective_id=0, has_side_effects=True, vmem_limit_bytes=66_000_000
        ),
        name="layer_back",
    )(
        grad_out, layer_inputs[0], gain_full, turned, rows, saved_gate[0], saved_up[0],
        w_down[0], w_gate[0], w_up[0], rp,
    )
    return grads[None]


def solution(mesh):
    placed = (
        P("section", None, "expert", "tensor"),
        P(None, "expert", "tensor"),
        P("section", "tensor"),
        P("section", "tensor", None),
        P("section", None, ("expert", "tensor")),
        P("section", None, ("expert", "tensor")),
        P("section", ("expert", "tensor"), None),
        P("section", None, None, None, ("expert", "tensor")),
        P("section", None, None, None, ("expert", "tensor")),
        P("section", None, "expert", None),
    )
    return jax.shard_map(
        on_device,
        mesh=mesh,
        in_specs=placed,
        out_specs=P("section", None, "expert", "tensor"),
        check_vma=False,
    )
```

```python
import functools
import jax
import jax.numpy as jnp
from jax import lax
from jax.experimental import pallas as pl
from jax.experimental.pallas import tpu as pltpu
from jax.sharding import PartitionSpec as P

norm_eps = 1e-05
OFF = (0, -1, 1, 2)
MESH = pl.DeviceIdType.MESH
NT = (((1,), (1,)), ((), ()))


def kernel(
    sections, n, sizes,
    gout, xin, gain_in, rt_in, rows_in, sg_h, su_h, wd_h, wg_h, wu_h,
    out,
    G, U, D, RH, RF, RHF, RFF, RX, hop, mrecv, msend,
    V, A, B, bt, DC, wd, wc, info, sg, su,
    xo, gain, gain_o, rp, ps, pr, tot, GI, tmp,
    ld, x_s, x_r, fo_s, fo_r, ff_s, ff_r, so_s, so_r, sf_s, sf_r, dd_s, dd_r,
    e_s, e_r, rh_s, rh_r, rf_s, rf_r, hf_s, hf_r, ff2_s, ff2_r, rx_s, rx_r,
    m_s, m_r, hop_s, hop_r, xo_s, xo_r, go_s, go_r, rp_s, rp_r, ps_s, ps_r, y_s, y_r, z_s, z_r, gate,
):
    micros, T, Q, F, cap, lanes = sizes
    width = 4 * Q
    K = 2 * F + lanes
    sec = lax.axis_index("section")
    ex = lax.axis_index("expert")
    te = lax.axis_index("tensor")
    z, y = ex // n, ex % n
    xl, c = te // 2, te % 2
    fp = y * (1 - c) + z * c
    sp = z * (1 - c) + y * c

    def at(v, o):
        return lax.rem(v + o + n, n)

    def exid(f, s):
        return (1 - c) * (s * n + f) + c * (f * n + s)

    partner = {"tensor": xl * 2 + 1 - c}
    xnbr = {"tensor": (1 - xl) * 2 + c}
    xdiag = {"tensor": (1 - xl) * 2 + 1 - c}
    fdir = ({"expert": exid(at(fp, 1), sp)}, {"expert": exid(at(fp, -1), sp)})
    sdir = ({"expert": exid(fp, at(sp, 1))}, {"expert": exid(fp, at(sp, -1))})
    across = (partner, xnbr, xdiag)
    ypeer = tuple({"expert": z * n + at(y, o)} for o in (1, 2, 3))
    zpeer = tuple({"expert": at(z, o) * n + y} for o in (1, 2, 3))
    hoppeer = {"section": 1 - sec, "tensor": (1 - xl) * 2 + c}
    near = across + fdir + sdir

    def load(k, src, dst):
        return pltpu.make_async_copy(src, dst, ld.at[k])

    def weight_loads():
        return (
            load(0, wd_h, wd),
            load(1, wg_h, wc.at[:, pl.ds(0, F)]),
            load(2, wu_h, wc.at[:, pl.ds(F, F)]),
        )

    for cp in weight_loads():
        cp.start()

    barrier = pltpu.get_barrier_semaphore()
    greeted = across + ypeer + zpeer + ((hoppeer,) if sections == 2 else ())
    for peer in greeted:
        pl.semaphore_signal(barrier, inc=1, device_id=peer, device_id_type=MESH)
    pl.semaphore_wait(barrier, len(greeted))

    def rc(src, dst, ss, rs, peer):
        return pltpu.make_async_remote_copy(
            src_ref=src, dst_ref=dst, send_sem=ss, recv_sem=rs, device_id=peer, device_id_type=MESH
        )

    def send(src, dst, ss, rs, peer):
        rc(src, dst, ss, rs, peer).start()

    def arrived(ref, ss, rs, peer):
        rc(ref, ref, ss, rs, peer).wait_recv()

    def tensor_parts():
        ps[...] = jnp.zeros_like(ps)
        gain[...] = gain_in[...].astype(jnp.float32)
        at_lane = lax.broadcasted_iota(jnp.int32, (lanes, 16), 0)
        spaced = at_lane == 48 + 16 * lax.broadcasted_iota(jnp.int32, (lanes, 16), 1)
        spaced = jnp.where(spaced, 1.0, 0.0).astype(jnp.bfloat16)
        router = lax.dot_general(
            rt_in[...], spaced, (((0,), (1,)), ((), ())), preferred_element_type=jnp.float32
        ).astype(jnp.bfloat16)
        rp[...] = router
        wc[pl.ds(pl.multiple_of(te * Q, Q), Q), 2 * F :] = router
        gr = rt_in[...].astype(jnp.float32) * gain[...]
        hi = gr.astype(jnp.bfloat16)
        lo = (gr - hi.astype(jnp.float32)).astype(jnp.bfloat16)
        ones = jnp.ones((16, Q), jnp.bfloat16)
        row = lax.broadcasted_iota(jnp.int32, (8, T), 0)

        def nt(a, b):
            return lax.dot_general(a, b, NT, preferred_element_type=jnp.float32)

        for m in range(micros):
            x = xin[m]
            sq = x.astype(jnp.float32) * x.astype(jnp.float32)
            h = sq.astype(jnp.bfloat16)
            low = (sq - h.astype(jnp.float32)).astype(jnp.bfloat16)
            logit = nt(hi, x) + nt(lo, x)
            total = nt(ones, h) + nt(ones, low)
            ps[m, :, 0:T] = jnp.where(row == 4, total[0:8], logit[0:8])
        for i, peer in enumerate(across):
            send(ps, pr.at[i], ps_s.at[i], ps_r.at[i], peer)

    def spread_inputs():
        send(xin, xo, xo_s, xo_r, xnbr)
        send(gain, gain_o, go_s, go_r, xnbr)
        for i, peer in enumerate(across):
            place = wc.at[pl.ds(pl.multiple_of(te * Q, Q), Q), pl.ds(2 * F, lanes)]
            send(rp, place, rp_s.at[i], rp_r.at[i], peer)

    def route_rows():
        for i, peer in enumerate(across):
            arrived(pr.at[i], ps_s.at[i], ps_r.at[i], peer)
        for m in range(micros):
            tot[m] = (ps[m] + pr[0, m]) + (pr[1, m] + pr[2, m])
            sc = lax.rsqrt(tot[m, 4:5] / width + norm_eps)
            e0, e1 = rows_in[m, 0:1], rows_in[m, 1:2]
            delta = jnp.zeros_like(sc)
            for k in range(4):
                pick = jnp.where(e0 == k, 1.0, 0.0) - jnp.where(e1 == k, 1.0, 0.0)
                delta = delta + pick * (tot[m, k : k + 1] * sc)
            GI[z, y, m, 0:1] = e0
            GI[z, y, m, 1:2] = e1
            GI[z, y, m, 2:3] = delta
            GI[z, y, m, 3:4] = sc
        for i, peer in enumerate(ypeer):
            send(GI.at[z, y], GI.at[z, y], y_s.at[i], y_r.at[i], peer)

    def rows_along_y():
        for i in range(3):
            arrived(GI.at[z, at(y, -1 - i)], y_s.at[i], y_r.at[i], ypeer[i])
        for i, peer in enumerate(zpeer):
            send(GI.at[z], GI.at[z], z_s.at[i], z_r.at[i], peer)

    def rows_along_z():
        for i in range(3):
            arrived(GI.at[at(z, -1 - i)], z_s.at[i], z_r.at[i], zpeer[i])
        own = z.astype(jnp.float32)
        before = lax.broadcasted_iota(jnp.int32, (lanes, lanes), 0) < lax.broadcasted_iota(
            jnp.int32, (lanes, lanes), 1
        )
        before = jnp.where(before, 1.0, 0.0).astype(jnp.bfloat16)
        for m in range(micros):
            for j in range(n * n):
                for r in range(4):
                    tmp[r, j : j + 1] = GI[j // n, j % n, m, r : r + 1]
            e0, e1, delta = tmp[0], tmp[1], tmp[2]
            is0 = jnp.where(e0 == own, 1.0, 0.0)
            is1 = jnp.where(e1 == own, 1.0, 0.0)
            used = is0 + is1
            pos = jnp.dot(used.astype(jnp.bfloat16), before, preferred_element_type=jnp.float32)
            pos = jnp.where(used > 0.5, pos, -1.0)
            q0, q1 = jax.nn.sigmoid(delta), jax.nn.sigmoid(-delta)
            parts = [pos, is0 * q0 + is1 * q1, is0 * q1 - is1 * q0]
            for k in range(4):
                parts.append(jnp.where(e0 == k, 1.0, 0.0) - jnp.where(e1 == k, 1.0, 0.0))
            parts.append(tmp[3])
            turned = jnp.concatenate(parts, axis=0).T[0:T]
            for j in range(n * n):
                info[m, j // n, j % n] = pltpu.roll(turned, (lanes - j) % lanes, 1)

    def finish_prologue():
        arrived(xo, xo_s, xo_r, xnbr)
        arrived(gain_o, go_s, go_r, xnbr)
        for i, o in enumerate((xl * 2 + 1 - c, (1 - xl) * 2 + c, (1 - xl) * 2 + 1 - c)):
            place = wc.at[pl.ds(pl.multiple_of(o * Q, Q), Q), pl.ds(2 * F, lanes)]
            arrived(place, rp_s.at[i], rp_r.at[i], across[i])
        rc(xin, xo, xo_s, xo_r, xnbr).wait_send()
        rc(gain, gain_o, go_s, go_r, xnbr).wait_send()
        for i, peer in enumerate(across):
            place = wc.at[pl.ds(pl.multiple_of(te * Q, Q), Q), pl.ds(2 * F, lanes)]
            rc(rp, place, rp_s.at[i], rp_r.at[i], peer).wait_send()
            rc(ps, pr.at[i], ps_s.at[i], ps_r.at[i], peer).wait_send()
        for i, peer in enumerate(ypeer):
            rc(GI.at[z, y], GI.at[z, y], y_s.at[i], y_r.at[i], peer).wait_send()
        for i, peer in enumerate(zpeer):
            rc(GI.at[z], GI.at[z], z_s.at[i], z_r.at[i], peer).wait_send()

    def one_micro(m, carry):
        @pl.when(m > 0)
        def _():
            for peer in near:
                pl.semaphore_signal(gate, inc=1, device_id=peer, device_id_type=MESH)
            pl.semaphore_wait(gate, len(near))

        small = (
            load(4, sg_h.at[m], sg),
            load(5, su_h.at[m], su),
        )
        for cp in small:
            cp.start()
        sent = []

        def go(*a):
            cp = rc(*a)
            cp.start()
            sent.append(cp)

        def got(ref, ss, rs, peer):
            rc(ref, ref, ss, rs, peer).wait_recv()

        top = sec == sections - 1
        ahead = jnp.logical_and(m == 0, jnp.logical_not(top))

        def first(f):
            pl.when(jnp.logical_and(m == 0, top))(f)

        def prepare(j, carry):
            i0, i1 = j // n, j % n
            pos = info[m, i0, i1, :, 0:1]
            slots = lax.broadcasted_iota(jnp.int32, (T, cap), 1).astype(jnp.float32)
            place = jnp.where(slots == pos, 1.0, 0.0).astype(jnp.bfloat16)
            a = jnp.dot(place, sg[j], preferred_element_type=jnp.float32)
            b = jnp.dot(place, su[j], preferred_element_type=jnp.float32)
            sig = jax.nn.sigmoid(a)
            A[i0, i1] = b * sig * (1.0 + a * (1.0 - sig))
            B[i0, i1] = a * sig
            bt[i0, i1] = b.astype(jnp.bfloat16)
            return carry

        def prepare_rows(i):
            @pl.when(jnp.logical_not(ahead))
            def _():
                lax.fori_loop(i * n, (i + 1) * n, prepare, 0)

        if sections == 2:

            @pl.when(ahead)
            def _():
                tensor_parts()
                spread_inputs()
                route_rows()
                rows_along_y()
                rows_along_z()
                for cp in small:
                    cp.wait()
                for cp in weight_loads():
                    cp.wait()
                finish_prologue()
                lax.fori_loop(0, n * n, prepare, 0)

        qh = jnp.where(top, xl, 1 - xl)
        qo = 1 - qh
        mine = G.at[c, sp, fp]

        @pl.when(top)
        def _():
            G[c, sp, fp, qh] = gout[m]

        if sections == 2:

            @pl.when(jnp.logical_not(top))
            def _():
                got(hop.at[m], hop_s.at[m], hop_r.at[m], hoppeer)
                G[c, sp, fp, qh] = hop[m]

        go(mine.at[qh], mine.at[qh], x_s, x_r, xnbr)
        for d in range(2):
            go(mine.at[qh], mine.at[qh], fo_s.at[0, d], fo_r.at[0, d], fdir[d])
        def spread(k, i, piece):
            for d in range(2):
                go(piece, piece, so_s.at[k, i, d], so_r.at[k, i, d], sdir[d])

        def forward(piece, ss, rs, peer):
            cp = rc(piece, piece, ss, rs, peer)
            sent.append(cp)
            return cp.start

        spread(0, 0, mine.at[qh])
        first(tensor_parts)
        V[...] = jnp.zeros_like(V)
        msend[...] = jnp.zeros_like(msend)
        got(mine.at[qo], x_s, x_r, xnbr)
        for d in range(2):
            go(mine.at[qo], mine.at[qo], fo_s.at[1, d], fo_r.at[1, d], fdir[d])
        spread(0, 1, mine.at[qo])

        def share(kk, k, slot):
            go(slot, slot, dd_s.at[kk, k], dd_r.at[kk, k], partner)

        share(0, 0, mine)
        first(spread_inputs)
        first(route_rows)

        @pl.when(jnp.logical_not(ahead))
        def _():
            for cp in small:
                cp.wait()

        @first
        def _():
            for cp in weight_loads():
                cp.wait()

        def half_v(kk, h):
            zi, yi = at(z, OFF[kk]), at(y, OFF[kk])
            part = jnp.zeros((n * T, F), jnp.float32)
            for q in range(2):
                g = (G[0, zi, :, q] if h == 0 else G[1, yi, :, q]).reshape(n * T, Q)
                w = wd[:, (2 * q + h) * Q : (2 * q + h + 1) * Q]
                part = part + lax.dot_general(g, w, NT, preferred_element_type=jnp.float32)
            part = part.reshape(n, T, F)
            if h == 0:
                V[zi] += part
            else:
                V[:, yi] += part

        def v_shared(kk):
            for k in range(n):
                ref = G.at[1 - c, at(fp, OFF[kk]), at(sp, OFF[k])]
                got(ref, dd_s.at[kk, k], dd_r.at[kk, k], partner)

        def into_v(kk):
            v_shared(kk)
            for h in range(2):
                half_v(kk, h)

        fslot = tuple(G.at[c, sp, at(fp, o)] for o in (-1, 1))
        fnext = [
            forward(fslot[d].at[d], ff_s.at[d], ff_r.at[d], fdir[d]) for d in range(2)
        ]
        for i, q in enumerate((qh, qo)):
            for d in range(2):
                got(fslot[d].at[q], fo_s.at[i, d], fo_r.at[i, d], fdir[d])
                pl.when(q == d)(fnext[d])
                spread(1 + d, i, fslot[d].at[q])
        for d in range(2):
            share(0, 1 + d, fslot[d])
        first(rows_along_y)
        far = G.at[c, sp, at(fp, 2)]
        for d in range(2):
            got(far.at[d], ff_s.at[d], ff_r.at[d], fdir[d])
            spread(3, d, far.at[d])
        share(0, 3, far)

        def pass_on(k):
            f = at(fp, OFF[k])
            slots = tuple(G.at[c, at(sp, o), f] for o in (-1, 1))
            nexts = [
                forward(slots[d].at[d], sf_s.at[k, d], sf_r.at[k, d], sdir[d]) for d in range(2)
            ]
            for i, q in enumerate((qh, qo) if k < 3 else (0, 1)):
                for d in range(2):
                    got(slots[d].at[q], so_s.at[k, i, d], so_r.at[k, i, d], sdir[d])
                    if k < 3:
                        pl.when(q == d)(nexts[d])
                    elif q == d:
                        nexts[d]()
            for d in range(2):
                share(1 + d, k, slots[d])

        first(rows_along_z)
        pass_on(0)
        prepare_rows(0)
        pass_on(1)
        into_v(0)
        prepare_rows(1)
        pass_on(2)
        prepare_rows(2)
        pass_on(3)
        prepare_rows(3)
        first(finish_prologue)
        for k in range(n):
            slot = G.at[c, at(sp, 2), at(fp, OFF[k])]
            for d in range(2):
                got(slot.at[d], sf_s.at[k, d], sf_r.at[k, d], sdir[d])
            share(3, k, slot)
            if k == 1:
                into_v(1)
            if k == 2:
                into_v(2)

        def finish(i0, i1):
            v = V[i0, i1]
            db = v * B[i0, i1]
            w = jnp.sum(db * bt[i0, i1].astype(jnp.float32), axis=-1, keepdims=True)
            row = info[m, i0, i1]
            DC[i0, i1, :, 0:F] = (v * A[i0, i1]).astype(jnp.bfloat16)
            DC[i0, i1, :, F : 2 * F] = db.astype(jnp.bfloat16)
            DC[i0, i1, :, 2 * F :] = (w * row[:, 32:33] * row).astype(jnp.bfloat16)

        def finish_near(j, carry):
            i, k = j // 3, j % 3
            finish(at(z, i + i // 2), at(y, k + k // 2))
            return carry

        def finish_far(j, carry):
            o, p = ((2, 0), (2, 1), (2, 2), (2, 3), (0, 2), (1, 2), (3, 2))[j]
            finish(at(z, o), at(y, p))
            return carry

        lax.fori_loop(0, 9, finish_near, 0)
        for core in range(2):
            pl.when(c == core)(functools.partial(half_v, 3, core))
        v_shared(3)
        for core in range(2):
            pl.when(c == core)(functools.partial(half_v, 3, 1 - core))
        for j in range(7):
            finish_far(j, 0)

        def half_u(blocks, h, q):
            da = jnp.concatenate([DC[i, k] for i, k in blocks], axis=0)
            q_own = jnp.concatenate([info[m, i, k, :, 16:17] for i, k in blocks], axis=0)
            w = wc[pl.ds(pl.multiple_of((2 * q + h) * Q, Q), Q), :]
            u = lax.dot_general(da, w, NT, preferred_element_type=jnp.float32)
            u = (u * q_own).astype(jnp.bfloat16)
            for j, (i, k) in enumerate(blocks):
                U[h, i * (1 - h) + k * h, k * (1 - h) + i * h, q] = u[j * T : (j + 1) * T]

        def unit(kk, q):
            zi, yi = at(z, OFF[kk]), at(y, OFF[kk])
            for h in (1 - c, c):
                rows = [(zi * (1 - h) + r * h, r * (1 - h) + yi * h) for r in range(n)]
                half_u(rows, h, q)
                if h is not c:
                    piece = U.at[1 - c, at(fp, OFF[kk]), :, q]
                    go(piece, D.at[kk, :, q], e_s.at[kk, q], e_r.at[kk, q], partner)

        def add_partner(kk, q):
            got(D.at[kk, :, q], e_s.at[kk, q], e_r.at[kk, q], partner)
            i = at(sp, OFF[kk])
            U[c, i, :, q] = U[c, i, :, q] + D[kk, :, q]

        s2 = at(sp, 2)
        for d in range(2):
            unit(3, d)
            add_partner(3, d)
            for k in (3, 2, 1, 0):
                go(U.at[c, s2, at(fp, OFF[k]), d], RH.at[d, k], rh_s.at[d, k], rh_r.at[d, k], sdir[d])

        def to_owner(d, k, q):
            i, f = at(sp, 1 if d == 0 else -1), at(fp, OFF[k])
            go(U.at[c, i, f, q], RF.at[d, k, q], rf_s.at[d, k, q], rf_r.at[d, k, q], sdir[d])

        for d in range(2):
            unit(2 - d, 1 - d)
            add_partner(2 - d, 1 - d)
            for k in (3, 2, 1, 0):
                to_owner(d, k, 1 - d)
        for d in range(2):
            unit(2 - d, d)
            add_partner(2 - d, d)

        def pass_sum(k):
            for d in range(2):
                i, f = at(sp, 1 if d == 0 else -1), at(fp, OFF[k])
                got(RH.at[d, k], rh_s.at[d, k], rh_r.at[d, k], sdir[d])
                U[c, i, f, d] = U[c, i, f, d] + RH[d, k]
                to_owner(d, k, d)

        pass_sum(3)
        pass_sum(2)
        unit(0, 0)
        pass_sum(1)
        pass_sum(0)
        unit(0, 1)
        for q in range(2):
            add_partner(0, q)

        def own_sum(k, q):
            for d in range(2):
                got(RF.at[d, k, q], rf_s.at[d, k, q], rf_r.at[d, k, q], sdir[d])
            f = at(fp, OFF[k])
            total = U[c, sp, f, q].astype(jnp.float32) + RF[0, k, q].astype(jnp.float32)
            U[c, sp, f, q] = (total + RF[1, k, q].astype(jnp.float32)).astype(jnp.bfloat16)

        f2 = at(fp, 2)
        for d in range(2):
            own_sum(3, d)
            go(U.at[c, sp, f2, d], RHF.at[d], hf_s.at[d], hf_r.at[d], fdir[d])
        for d, k in ((0, 2), (1, 1)):
            f = at(fp, OFF[k])
            for q in range(2):
                own_sum(k, q)
            got(RHF.at[d], hf_s.at[d], hf_r.at[d], fdir[d])
            U[c, sp, f, d] = U[c, sp, f, d] + RHF[d]
            for i, q in enumerate((1 - xl, xl)):
                go(U.at[c, sp, f, q], RFF.at[d, q], ff2_s.at[d, i], ff2_r.at[d, i], fdir[d])
        for q in range(2):
            own_sum(0, q)

        def three(i, q):
            for d in range(2):
                got(RFF.at[d, q], ff2_s.at[d, i], ff2_r.at[d, i], fdir[d])
            total = U[c, sp, fp, q].astype(jnp.float32) + RFF[0, q].astype(jnp.float32)
            return total + RFF[1, q].astype(jnp.float32)

        other = three(0, 1 - xl)
        U[c, sp, fp, 1 - xl] = other.astype(jnp.bfloat16)
        go(U.at[c, sp, fp, 1 - xl], RX, rx_s, rx_r, xnbr)
        dn = three(1, xl)

        values = xin[m].astype(jnp.float32)
        both = values * (dn * gain[...]) + xo[m].astype(jnp.float32) * (other * gain_o[...])
        high = both.astype(jnp.bfloat16)
        low = (both - high.astype(jnp.float32)).astype(jnp.bfloat16)
        ones = jnp.ones((8, Q), jnp.bfloat16)
        msend[:, 0:T] = lax.dot_general(
            ones, high, NT, preferred_element_type=jnp.float32
        ) + lax.dot_general(ones, low, NT, preferred_element_type=jnp.float32)
        for i, peer in enumerate(across):
            go(msend, mrecv.at[i], m_s.at[i], m_r.at[i], peer)
        got(RX, rx_s, rx_r, xnbr)
        gained = (dn + RX[...].astype(jnp.float32)) * gain[...]
        for i, peer in enumerate(across):
            got(mrecv.at[i], m_s.at[i], m_r.at[i], peer)
        moment = ((msend[...] + mrecv[0]) + (mrecv[1] + mrecv[2])).T[0:T, 0:1] / width
        sc = info[m, z, y, :, 112:113]
        result = G[c, sp, fp, xl].astype(jnp.float32) + sc * gained - values * (sc * sc * sc * moment)
        out[m] = result.astype(jnp.bfloat16)
        if sections == 2:

            @pl.when(top)
            def _():
                rc(out.at[m], hop.at[m], hop_s.at[m], hop_r.at[m], hoppeer).start()

        for cp in sent:
            cp.wait_send()
        if sections == 2:

            @pl.when(top)
            def _():
                rc(out.at[m], hop.at[m], hop_s.at[m], hop_r.at[m], hoppeer).wait_send()

        return carry

    lax.fori_loop(0, micros, one_micro, 0)


def on_device(
    layer_inputs, grad_out, norm_gain, router_w, w_gate, w_up, w_down, saved_gate, saved_up, routes
):
    sections = lax.axis_size("section")
    n = 4
    micros, T, Q = grad_out.shape
    F = w_gate.shape[2]
    cap = saved_gate.shape[3]
    lanes = 128
    router = router_w[0]
    experts = router.shape[1]
    width = w_gate.shape[1]
    turned = jnp.pad(router.T, ((0, 16 - experts), (0, 0)))
    rows = jnp.swapaxes(routes[0], 1, 2).astype(jnp.float32)
    rows = jnp.pad(rows, ((0, 0), (0, 6), (0, lanes - T)), constant_values=-5.0)

    bf, f32 = jnp.bfloat16, jnp.float32
    vm = pl.BlockSpec(memory_space=pltpu.VMEM)
    anym = pl.BlockSpec(memory_space=pl.ANY)
    dma = pltpu.SemaphoreType.DMA
    K = 2 * F + lanes
    grads = pl.pallas_call(
        functools.partial(kernel, sections, n, (micros, T, Q, F, cap, lanes)),
        out_shape=jax.ShapeDtypeStruct((micros, T, Q), bf),
        in_specs=[vm] * 5 + [anym] * 5,
        out_specs=vm,
        scratch_shapes=[
            pltpu.VMEM((2, n, n, 2, T, Q), bf),
            pltpu.VMEM((2, n, n, 2, T, Q), bf),
            pltpu.VMEM((n, n, 2, T, Q), bf),
            pltpu.VMEM((2, n, T, Q), bf),
            pltpu.VMEM((2, n, 2, T, Q), bf),
            pltpu.VMEM((2, T, Q), bf),
            pltpu.VMEM((2, 2, T, Q), bf),
            pltpu.VMEM((T, Q), bf),
            pltpu.VMEM((micros, T, Q), bf),
            pltpu.VMEM((3, 8, lanes), f32),
            pltpu.VMEM((8, lanes), f32),
            pltpu.VMEM((n, n, T, F), f32),
            pltpu.VMEM((n, n, T, F), f32),
            pltpu.VMEM((n, n, T, F), f32),
            pltpu.VMEM((n, n, T, F), bf),
            pltpu.VMEM((n, n, T, K), bf),
            pltpu.VMEM((F, width), bf),
            pltpu.VMEM((width, K), bf),
            pltpu.VMEM((micros, n, n, T, lanes), f32),
            pltpu.VMEM((n * n, cap, F), bf),
            pltpu.VMEM((n * n, cap, F), bf),
            pltpu.VMEM((micros, T, Q), bf),
            pltpu.VMEM((1, Q), f32),
            pltpu.VMEM((1, Q), f32),
            pltpu.VMEM((Q, lanes), bf),
            pltpu.VMEM((micros, 8, lanes), f32),
            pltpu.VMEM((3, micros, 8, lanes), f32),
            pltpu.VMEM((micros, 8, lanes), f32),
            pltpu.VMEM((n, n, micros, 8, lanes), f32),
            pltpu.VMEM((4, n * n, lanes), f32),
            dma((6,)),
            dma, dma,
            dma((2, 2)), dma((2, 2)), dma((2,)), dma((2,)),
            dma((4, 2, 2)), dma((4, 2, 2)), dma((4, 2)), dma((4, 2)),
            dma((4, 4)), dma((4, 4)),
            dma((4, 2)), dma((4, 2)), dma((2, 4)), dma((2, 4)), dma((2, 4, 2)), dma((2, 4, 2)),
            dma((2,)), dma((2,)), dma((2, 2)), dma((2, 2)), dma, dma,
            dma((3,)), dma((3,)), dma((micros,)), dma((micros,)),
            dma, dma, dma, dma, dma((3,)), dma((3,)), dma((3,)), dma((3,)),
            dma((3,)), dma((3,)), dma((3,)), dma((3,)),
            pltpu.SemaphoreType.REGULAR,
        ],
        compiler_params=pltpu.CompilerParams(
            collective_id=0, has_side_effects=True, vmem_limit_bytes=66_000_000
        ),
        name="layer_back",
    )(
        grad_out, layer_inputs[0], norm_gain, turned, rows, saved_gate[0], saved_up[0],
        w_down[0], w_gate[0], w_up[0],
    )
    return grads[None]


def solution(mesh):
    placed = (
        P("section", None, "expert", "tensor"),
        P(None, "expert", "tensor"),
        P("section", "tensor"),
        P("section", "tensor", None),
        P("section", None, ("expert", "tensor")),
        P("section", None, ("expert", "tensor")),
        P("section", ("expert", "tensor"), None),
        P("section", None, None, None, ("expert", "tensor")),
        P("section", None, None, None, ("expert", "tensor")),
        P("section", None, "expert", None),
    )
    return jax.shard_map(
        on_device,
        mesh=mesh,
        in_specs=placed,
        out_specs=P("section", None, "expert", "tensor"),
        check_vma=False,
    )
```
